32 devices in a mesh: ep: 8 (over y, x, core), tp: 4 (over z).
Axes of the slice: x: 2, y: 2, z: 4, core: 2. Of those that a mesh axis runs over, the one named last changes fastest.
Arguments:
- tokens: bfloat16 [2048, 7168], P('ep', 'tp'), may hold values from -78 to 78
- norm_gain: bfloat16 [7168], P('tp'), may hold values from 0.5 to 1.5
- expert_ids: int32 [2048, 8], P('ep'), may hold values from 0 to 63, all different within a row
- gate_prob: bfloat16 [2048, 8], P('ep'), may hold values from 0.049804688 to 1
- w_gate: bfloat16 [8, 7168, 2048], P('ep', None, 'tp'), may hold values from -0.0625 to 0.0625
- w_up: bfloat16 [8, 7168, 2048], P('ep', None, 'tp'), may hold values from -0.0625 to 0.0625
- w_down: bfloat16 [8, 2048, 7168], P('ep', 'tp'), may hold values from -0.125 to 0.125
Outputs:
- combined: bfloat16 [2048, 7168], P('ep', 'tp')
The draws below stay inside these ranges and needn't reach their ends.
Inputs may be any that keep to these rules, and one draw needn't show every extreme that they name: `expert_ids`: each row names 8 different experts.
All inputs are finite; a program needn't handle non-finite values.
Results may differ from the reference program's by a relative error of at most 0.01.
Values may be sent and summed in bfloat16 or wider, within the bound.
A program may use at most 128 MiB of HBM per device.

```python
import math
import jax
import jax.numpy as jnp
from jax import lax

D = 7168
FF = 2048
TOP = 8
TOK_DEV = 256
EXPERTS = 64
WINDOW = 8
TOKENS = 2048
CAP = 64
N_TP = 4


def draw_tokens(key, part):
    base_key = jax.random.fold_in(key, 11)
    row_key = jax.random.fold_in(key, 12)
    col_key = jax.random.fold_in(key, 13)
    rows_scale = jnp.exp(jax.random.uniform(row_key, (TOKENS, 1), jnp.float32, math.log(0.3), math.log(3.0)))
    rising = 3.0 ** (jnp.arange(D, dtype=jnp.float32) / D - 0.5)
    cols_scale = rising * jnp.exp(jax.random.uniform(col_key, (D,), jnp.float32, math.log(0.4), math.log(2.5)))
    base = jnp.clip(jax.random.normal(base_key, (TOKENS, D), jnp.float32), -6.0, 6.0)
    return (base * rows_scale * cols_scale[None, :]).astype(jnp.bfloat16)


def block_levels(key, shape, pieces, low, largest):
    def one(dim, shards_of):
        heights = jax.random.uniform(jax.random.fold_in(jax.random.fold_in(key, 6), dim), (shards_of,), jnp.float32, low / len(pieces), largest / len(pieces))
        return jnp.repeat(jnp.exp(heights), shape[dim] // shards_of).reshape((-1,) + (1,) * (len(shape) - dim - 1))

    factor_of = one(*pieces[0])
    for cut in pieces[1:]:
        factor_of = factor_of * one(*cut)
    return factor_of


def distinct(own_key, rows, amount, top, lift):
    sequence = jax.random.permutation(jax.random.fold_in(own_key, 1), amount)
    boost = sequence
    for power in range(3):
        boost = boost * boost // amount
    boost = boost * lift // amount
    lots = jax.random.randint(jax.random.fold_in(own_key, 2), (rows, amount), 0, 4096) + boost
    sure = jax.random.permutation(jax.random.fold_in(own_key, 3), rows)[jnp.arange(amount) % rows]
    lots = jnp.where(jnp.arange(rows)[:, None] == sure[None, :], 1 << 14, lots)
    score = lots * amount + jnp.arange(amount)
    return lax.top_k(score.astype(jnp.int32), top)[1].astype(jnp.int32)


def noise(own_key, shape, width, reach, shards=(), kind=jnp.bfloat16):
    array = jax.random.normal(own_key, shape, jnp.float32) * width
    if len(shards) > 0:
        array = block_levels(own_key, shape, shards, -0.22, 0.18) * array
    return jnp.clip(array, min=-reach, max=reach).astype(kind)


def setup_inputs(seed: int = 0) -> dict:
    arg_keys = jax.random.split(jax.random.key(seed), 8)
    tokens = draw_tokens(jax.random.fold_in(arg_keys[7], 71), 0)
    norm_gain = jnp.clip(1.0 + 0.1 * jax.random.normal(arg_keys[1], (D,), jnp.float32), 0.5, 1.5).astype(jnp.bfloat16)
    expert_ids = distinct(arg_keys[2], TOKENS, EXPERTS, TOP, 2048)
    gate_prob = jnp.clip(jnp.exp(math.log(1.0) - 2.9996462 * jax.random.uniform(arg_keys[3], (TOKENS, TOP), jnp.float32) ** block_levels(arg_keys[3], (TOKENS, TOP), ((0, 8),), -0.2, 0.2)), 0.049804688, 1.0).astype(jnp.bfloat16)
    w_gate = noise(arg_keys[4], (WINDOW, D, FF), D ** -0.5, 0.0625, ((0, 8), (2, 4)))
    w_up = noise(arg_keys[5], (WINDOW, D, FF), D ** -0.5, 0.0625, ((0, 8), (2, 4)))
    w_down = noise(arg_keys[6], (WINDOW, FF, D), FF ** -0.5, 0.125, ((0, 8), (1, 4)))
    return dict(tokens=tokens, norm_gain=norm_gain, expert_ids=expert_ids, gate_prob=gate_prob, w_gate=w_gate, w_up=w_up, w_down=w_down)


epsilon = 1e-06

def slots_of(expert_ids):
    is_live = expert_ids < WINDOW
    matches = (expert_ids[:, :, None] == jnp.arange(WINDOW, dtype=jnp.int32)).astype(jnp.int32)
    counts = lax.optimization_barrier(jnp.sum(matches, axis=1))
    blocked = counts.reshape(-1, TOK_DEV, WINDOW)
    before = (jnp.cumsum(blocked, axis=1) - blocked).reshape(-1, WINDOW)
    slot_index = lax.optimization_barrier(jnp.sum(matches * before[:, None, :], axis=2))
    is_kept = is_live & (slot_index < CAP)
    return (slot_index, is_kept)

def reference(tokens, norm_gain, expert_ids, gate_prob, w_gate, w_up, w_down):
    values = tokens.astype(jnp.float32)
    mean_square = lax.optimization_barrier(jnp.mean(values * values, axis=1, keepdims=True))
    normed = (values * lax.rsqrt(mean_square + epsilon) * norm_gain.astype(jnp.float32)).astype(jnp.bfloat16)
    slot_index, is_kept = slots_of(expert_ids)
    block_count = TOKENS // TOK_DEV
    block_index = (jnp.arange(TOKENS, dtype=jnp.int32) // TOK_DEV)[:, None]
    slot_total = WINDOW * block_count * CAP
    flat_index = jnp.where(is_kept, (expert_ids * block_count + block_index) * CAP + slot_index, slot_total).astype(jnp.int32)
    buffer = jnp.zeros((slot_total, D), jnp.bfloat16)
    for column in range(TOP):
        buffer = buffer.at[flat_index[:, column]].set(normed, mode='drop')
    buffer = buffer.reshape(WINDOW, block_count * CAP, D)
    block_width = FF // N_TP

    def one_expert(operands):
        rows_in, gate_matrix, up_matrix, down_matrix = operands
        gate_act = jnp.dot(rows_in, gate_matrix, preferred_element_type=jnp.float32)
        up_act = jnp.dot(rows_in, up_matrix, preferred_element_type=jnp.float32)
        hidden = (jax.nn.silu(gate_act) * up_act).astype(jnp.bfloat16)
        summed = jnp.zeros((rows_in.shape[0], D), jnp.float32)
        for block_number in range(N_TP):
            lower = block_number * block_width
            down_part = jnp.dot(hidden[:, lower:lower + block_width], down_matrix[lower:lower + block_width], preferred_element_type=jnp.float32)
            rounded = lax.optimization_barrier(down_part.astype(jnp.bfloat16))
            summed = summed + rounded.astype(jnp.float32)
        return summed.astype(jnp.bfloat16)
    expert_out = lax.map(one_expert, (buffer, w_gate, w_up, w_down)).reshape(slot_total, D)
    combined = jnp.zeros((TOKENS, D), jnp.float32)
    for column in range(TOP):
        picked = jnp.take(expert_out, flat_index[:, column], axis=0, mode='fill', fill_value=0).astype(jnp.float32)
        combined = combined + gate_prob[:, column:column + 1].astype(jnp.float32) * picked
    return combined.astype(jnp.bfloat16)
```

```python
import functools

import jax
import jax.numpy as jnp
from jax import lax
from jax.experimental import pallas as pl
from jax.experimental.pallas import tpu as pltpu
from jax.sharding import PartitionSpec as P

TOP = 8
EXP_DEV = 8
SHARE = 7
EPSILON = 1e-06
BF16 = jnp.bfloat16
F32 = jnp.float32


def look_up(table, index):
    span = len(table) ** 2
    total = 0
    for i, value in enumerate(table):
        if value:
            total = total + value * (1 - ((index - i) * (index - i) + span - 1) // span)
    return total


def near_first(n_tp):
    table = []
    for z in range(n_tp):
        inner = 1 if z < n_tp / 2 else -1
        table += sorted(range(n_tp), key=lambda s: (abs(s - z), -inner * (s - z)))
    return table


def body(
    n_ep, n_tp, rows, width, cap, wide, n_tok, n_slot,
    tok_hbm, gain_ref, ids_ref, prob_ref, gate_hbm, up_hbm, down_hbm,
    out_ref,
    tok, gains, stats, scale, dmat, wmat, send, recv, slot_in, w_gate, w_up, w_down,
    acc, hid, ret, ret_slot, in_tok, in_slot, part,
    load_sem, st_send, st_recv, zt_send, zt_recv, xs, xr, ys, yr, zp_send, zp_recv,
):
    e, z = lax.axis_index("ep"), lax.axis_index("tp")
    last = n_tp - 1
    items = n_tok + n_slot
    slots = n_ep * cap
    steps = n_tp * n_tok
    table = near_first(n_tp)

    def nth(k):
        return look_up(table, z * n_tp + k)

    def column(slice_index, item):
        return pl.multiple_of(slice_index * width + item * wide, wide)

    def remote(axis, index, src, dst, send_sem, recv_sem):
        return pltpu.make_async_remote_copy(
            src_ref=src,
            dst_ref=dst,
            send_sem=send_sem,
            recv_sem=recv_sem,
            device_id={axis: index},
            device_id_type=pl.DeviceIdType.MESH,
        )

    def each_peer(fn):
        def step(shift, carry):
            fn(lax.rem(e + shift, n_ep))
            return carry

        lax.fori_loop(1, n_ep, step, 0)

    loads = [
        pltpu.make_async_copy(
            tok_hbm.at[:, pl.ds(m * wide, wide)], tok.at[z, m], load_sem.at[m]
        )
        for m in range(items)
    ]
    weights = [
        pltpu.make_async_copy(src, dst, load_sem.at[items + i])
        for i, (src, dst) in enumerate(
            ((gate_hbm, w_gate), (up_hbm, w_up), (down_hbm, w_down))
        )
    ]
    for copy in loads + weights:
        copy.start()

    barrier = pltpu.get_barrier_semaphore()

    def greet(axis, index):
        pl.semaphore_signal(
            barrier, inc=1, device_id={axis: index}, device_id_type=pl.DeviceIdType.MESH
        )

    each_peer(lambda p: greet("ep", p))
    for shift in range(1, n_tp):
        greet("tp", lax.rem(z + shift, n_tp))

    ids = ids_ref[...]
    prob = prob_ref[...].astype(F32)
    lane = lax.broadcasted_iota(jnp.int32, (rows, 128), 1)
    picked = jnp.zeros((rows, 128), F32)
    chance = jnp.zeros((rows, 128), F32)
    for k in range(TOP):
        same = ids[:, k : k + 1] == lane
        picked = jnp.where(same, 1.0, picked)
        chance = jnp.where(same, prob[:, k : k + 1], chance)
    picked = picked.astype(BF16)
    earlier = (
        lax.broadcasted_iota(jnp.int32, (rows, rows), 1)
        < lax.broadcasted_iota(jnp.int32, (rows, rows), 0)
    )
    earlier = jnp.where(earlier, 1.0, 0.0).astype(BF16)
    before = jnp.dot(earlier, picked, preferred_element_type=F32).astype(BF16)
    spread_row = lax.broadcasted_iota(jnp.int32, (128, slots), 0)
    spread_col = lax.broadcasted_iota(jnp.int32, (128, slots), 1)
    spread = jnp.where(
        (spread_col >= spread_row * cap) & (spread_col < (spread_row + 1) * cap), 1.0, 0.0
    ).astype(BF16)
    is_picked = jnp.dot(picked, spread, preferred_element_type=F32)
    place = jnp.dot(before, spread, preferred_element_type=F32)
    weight = jnp.dot(chance.astype(BF16), spread, preferred_element_type=F32)
    position = lax.rem(lax.broadcasted_iota(jnp.int32, (rows, slots), 1), cap).astype(F32)
    hit = (is_picked > 0.5) & (place == position)
    wmat[...] = jnp.where(hit, weight, 0.0).astype(BF16)
    dmat[...] = jnp.where(hit, 1.0, 0.0).T.astype(BF16)

    square = jnp.zeros((rows, 1), F32)
    for m in range(items):
        loads[m].wait()
        values = tok[z, m].astype(F32)
        square = square + jnp.sum(values * values, axis=1, keepdims=True)
    stats[z] = jnp.broadcast_to(square, (rows, 128)).T[0:8, :]
    gains[z] = gain_ref[...]

    pl.semaphore_wait(barrier, n_ep - 1 + n_tp - 1)

    def share(shift):
        peer = lax.rem(z + shift, n_tp)
        return (
            remote("tp", peer, stats.at[z], stats.at[z], st_send.at[shift, 0], st_recv.at[shift, 0]),
            remote("tp", peer, gains.at[z], gains.at[z], st_send.at[shift, 1], st_recv.at[shift, 1]),
        )

    for shift in range(1, n_tp):
        for copy in share(shift):
            copy.start()

    def along(way, s, m, ref):
        peer = lax.rem(z + n_tp - 1 if way == 0 else z + 1, n_tp)
        return remote("tp", peer, ref, ref, zt_send.at[way, s, m], zt_recv.at[s, m])

    for m in range(n_tok):
        @pl.when(z > 0)
        def _():
            along(0, z, m, tok.at[z, m]).start()

        @pl.when(z < last)
        def _():
            along(1, z, m, tok.at[z, m]).start()

    for shift in range(1, n_tp):
        for copy in share(shift):
            copy.wait_recv()
    total = stats[0]
    for i in range(1, n_tp):
        total = total + stats[i]
    factor = lax.rsqrt(total / (width * n_tp) + EPSILON)
    scale[...] = jnp.broadcast_to(factor[0:1, :], (128, rows)).T

    def to_peers(index, dst, send_sem, recv_sem):
        own = pl.ds(pl.multiple_of(e * cap, cap), cap)
        dst[own, :] = send[index, own, :]

        def one(p):
            theirs = pl.ds(pl.multiple_of(p * cap, cap), cap)
            remote("ep", p, send.at[index, theirs, :], dst.at[own, :], send_sem, recv_sem).start()

        each_peer(one)

    def all_peers(index, dst, send_sem, recv_sem):
        most = pl.ds(0, (n_ep - 1) * cap)
        return remote(
            "ep", lax.rem(e + 1, n_ep), send.at[index, most, :], dst.at[most, :], send_sem, recv_sem
        )

    def dispatch(s, m, index, dst):
        gain = gains[s, :, pl.ds(pl.multiple_of(m * wide, wide), wide)]
        normed = tok[s, m].astype(F32) * scale[:, 0:1] * gain
        placed = jnp.dot(dmat[...], normed.astype(BF16), preferred_element_type=F32)
        send[index] = placed.astype(BF16)
        to_peers(index, dst, xs.at[index], xr.at[index])

    def gate_up(chunk, row, first=False):
        values = chunk[...]
        at = pl.ds(row, wide)
        for i, matrix in enumerate((w_gate, w_up)):
            product = jnp.dot(values, matrix[at, :], preferred_element_type=F32)
            acc[i] = product if first else acc[i] + product

    for a in range(n_slot):
        dispatch(z, n_tok + a, steps + a, slot_in.at[z, a])

    @pl.loop(0, n_tok)
    def _(j):
        dispatch(z, j, j, recv.at[j])

    weights[0].wait()
    weights[1].wait()
    for a in range(n_slot):
        all_peers(steps + a, slot_in.at[z, a], xs.at[steps + a], xr.at[steps + a]).wait_recv()

        @pl.when(z > 0)
        def _():
            along(0, z, n_tok + a, slot_in.at[z, a]).start()

        @pl.when(z < last)
        def _():
            along(1, z, n_tok + a, slot_in.at[z, a]).start()

        gate_up(slot_in.at[z, a], column(z, n_tok + a), first=a == 0)

    def arrive(k, m, ref_of):
        @pl.when(z + k <= last)
        def _():
            along(0, z + k, m, ref_of(z + k)).wait_recv()

            @pl.when(z > 0)
            def _():
                along(0, z + k, m, ref_of(z + k)).start()

        @pl.when(z - k >= 0)
        def _():
            along(1, z - k, m, ref_of(z - k)).wait_recv()

            @pl.when(z < last)
            def _():
                along(1, z - k, m, ref_of(z - k)).start()

    def take_in(index, s, m):
        all_peers(index, recv.at[index], xs.at[index], xr.at[index]).wait_recv()
        gate_up(recv.at[index], column(s, m))

    @pl.loop(n_tok, steps)
    def _(i):
        k, j = i // n_tok, i % n_tok
        arrive(k, j, lambda s: tok.at[s, j])
        dispatch(nth(k), j, i, recv.at[i])
        take_in(i - n_tok, nth(k - 1), j)
        for a in range(n_slot):
            @pl.when((j == n_tok - 1) & (k < last))
            def _():
                arrive(k, n_tok + a, lambda s: slot_in.at[s, a])

    for a in range(n_slot):
        @pl.loop(1, last)
        def _(k):
            s = nth(k)
            gate_up(slot_in.at[s, a], column(s, n_tok + a))

    @pl.loop(0, n_tok)
    def _(j):
        take_in(steps - n_tok + j, nth(last), j)

    for a in range(n_slot):
        arrive(last, n_tok + a, lambda s: slot_in.at[s, a])
        s = nth(last)
        gate_up(slot_in.at[s, a], column(s, n_tok + a))

    gate_act = acc[0]
    hid[...] = (gate_act / (1.0 + jnp.exp(-gate_act)) * acc[1]).astype(BF16)
    weights[2].wait()

    def down(index, s, m):
        matrix = w_down[:, pl.ds(column(s, m), wide)]
        send[index] = jnp.dot(hid[...], matrix, preferred_element_type=F32).astype(BF16)

    def onward(way, k, s, m, src, landing):
        peer = lax.rem(z + 1 if way == 0 else z + n_tp - 1, n_tp)
        return remote("tp", peer, src, landing.at[way, s], zp_send.at[k, m], zp_recv.at[way, s, m])

    for a in range(n_slot):
        all_peers(steps + a, slot_in.at[z, a], xs.at[steps + a], xr.at[steps + a]).wait_send()

    def far(k):
        return nth(last - k)

    for a in range(n_slot):
        @pl.loop(0, n_tp)
        def _(k):
            s, index = far(k), steps + k * n_slot + a
            down(index, s, n_tok + a)

            @pl.when((z == 0) & (k < last))
            def _():
                onward(0, k, s, n_tok + a, send.at[index], in_slot.at[a]).start()

            @pl.when((z == last) & (k < last))
            def _():
                onward(1, k, s, n_tok + a, send.at[index], in_slot.at[a]).start()

    @pl.loop(0, steps)
    def _(i):
        k, j = i // n_tok, i % n_tok
        all_peers(i, recv.at[i], xs.at[i], xr.at[i]).wait_send()
        down(i, far(k), j)
        to_peers(i, ret.at[i], ys.at[i], yr.at[i])

    for a in range(n_slot):
        @pl.loop(0, last)
        def _(k):
            s, index = far(k), steps + k * n_slot + a

            def pass_on(way):
                copy = onward(way, k, s, n_tok + a, send.at[index], in_slot.at[a])
                copy.wait_recv()
                summed = send[index].astype(F32) + in_slot[a, way, s].astype(F32)
                send[index] = summed.astype(BF16)
                copy.start()

            @pl.when((s > z) & (z > 0))
            def _():
                pass_on(0)

            @pl.when((s < z) & (z < last))
            def _():
                pass_on(1)

    def combine(i):
        all_peers(i, ret.at[i], ys.at[i], yr.at[i]).wait_recv()
        return jnp.dot(wmat[...], ret[i], preferred_element_type=F32)

    def add_in(way, s, j):
        landing = in_tok.at[j]
        onward(way, 0, s, j, landing.at[way, s], landing).wait_recv()
        part[...] = part[...] + in_tok[j, way, s].astype(F32)

    def forward_part(i):
        k, j = i // n_tok, i % n_tok
        s = far(k)
        part[...] = combine(i)

        @pl.when((s > z) & (z > 0))
        def _():
            add_in(0, s, j)

        @pl.when((s < z) & (z < last))
        def _():
            add_in(1, s, j)

        recv[i, 0:rows, :] = part[...].astype(BF16)

        @pl.when(s > z)
        def _():
            onward(0, k, s, j, recv.at[i, pl.ds(0, rows), :], in_tok.at[j]).start()

        @pl.when(s < z)
        def _():
            onward(1, k, s, j, recv.at[i, pl.ds(0, rows), :], in_tok.at[j]).start()

    @pl.loop(0, n_tok)
    def _(i):
        forward_part(i)

    for a in range(n_slot):
        index = steps + last * n_slot + a

        def add_slot(way):
            copy = onward(way, 0, z, n_tok + a, send.at[index], in_slot.at[a])
            copy.wait_recv()
            send[index] = (send[index].astype(F32) + in_slot[a, way, z].astype(F32)).astype(BF16)

        @pl.when(z > 0)
        def _():
            add_slot(0)

        @pl.when(z < last)
        def _():
            add_slot(1)

        to_peers(index, ret_slot.at[a], ys.at[steps + a], yr.at[steps + a])

    @pl.loop(n_tok, steps - n_tok)
    def _(i):
        forward_part(i)

    @pl.loop(0, n_tok)
    def _(j):
        part[...] = combine(steps - n_tok + j)

        @pl.when(z > 0)
        def _():
            add_in(0, z, j)

        @pl.when(z < last)
        def _():
            add_in(1, z, j)

        out_ref[:, pl.ds(pl.multiple_of(j * wide, wide), wide)] = part[...].astype(BF16)

    for a in range(n_slot):
        index = steps + last * n_slot + a
        all_peers(index, ret_slot.at[a], ys.at[steps + a], yr.at[steps + a]).wait_recv()
        m = n_tok + a
        out_ref[:, m * wide : (m + 1) * wide] = jnp.dot(
            wmat[...], ret_slot[a], preferred_element_type=F32
        ).astype(BF16)

    for shift in range(1, n_tp):
        for copy in share(shift):
            copy.wait_send()

    @pl.loop(0, n_tp)
    def _(s):
        @pl.when((z > 0) & (s >= z))
        def _():
            for m in range(items):
                ref = tok.at[s, m] if m < n_tok else slot_in.at[s, m - n_tok]
                along(0, s, m, ref).wait_send()

        @pl.when((z < last) & (s <= z))
        def _():
            for m in range(items):
                ref = tok.at[s, m] if m < n_tok else slot_in.at[s, m - n_tok]
                along(1, s, m, ref).wait_send()

    @pl.loop(0, steps)
    def _(i):
        all_peers(i, ret.at[i], ys.at[i], yr.at[i]).wait_send()

    for a in range(n_slot):
        index = steps + last * n_slot + a
        all_peers(index, ret_slot.at[a], ys.at[steps + a], yr.at[steps + a]).wait_send()

    @pl.loop(0, last)
    def _(k):
        for m in range(n_tok):
            onward(
                0, k, 0, m, recv.at[k * n_tok + m, pl.ds(0, rows), :], in_tok.at[m]
            ).wait_send()
        for a in range(n_slot):
            onward(
                0, k, 0, n_tok + a, send.at[steps + k * n_slot + a], in_slot.at[a]
            ).wait_send()


def local(tokens, norm_gain, expert_ids, gate_prob, w_gate, w_up, w_down):
    n_ep = lax.axis_size("ep")
    n_tp = lax.axis_size("tp")
    rows, width = tokens.shape
    cap = max(2, 2 * rows * TOP // (EXP_DEV * n_ep))
    slots = n_ep * cap
    wide = 256 if width % 256 == 0 else 128
    items = width // wide
    n_slot = max(1, items // SHARE)
    n_tok = items - n_slot
    units = w_gate.shape[2]
    steps = n_tp * n_tok

    kernel = functools.partial(body, n_ep, n_tp, rows, width, cap, wide, n_tok, n_slot)
    vmem = pl.BlockSpec(memory_space=pltpu.VMEM)
    hbm = pl.BlockSpec(memory_space=pl.ANY)
    dma = pltpu.SemaphoreType.DMA
    return pl.pallas_call(
        kernel,
        out_shape=jax.ShapeDtypeStruct((rows, width), BF16),
        in_specs=[hbm, vmem, vmem, vmem, hbm, hbm, hbm],
        out_specs=vmem,
        scratch_shapes=[
            pltpu.VMEM((n_tp, items, rows, wide), BF16),
            pltpu.VMEM((n_tp, 1, width), F32),
            pltpu.VMEM((n_tp, 8, rows), F32),
            pltpu.VMEM((rows, 128), F32),
            pltpu.VMEM((slots, rows), BF16),
            pltpu.VMEM((rows, slots), BF16),
            pltpu.VMEM((n_tp * items, slots, wide), BF16),
            pltpu.VMEM((steps, slots, wide), BF16),
            pltpu.VMEM((n_tp, n_slot, slots, wide), BF16),
            pltpu.VMEM((n_tp * width, units), BF16),
            pltpu.VMEM((n_tp * width, units), BF16),
            pltpu.VMEM((units, n_tp * width), BF16),
            pltpu.VMEM((2, slots, units), F32),
            pltpu.VMEM((slots, units), BF16),
            pltpu.VMEM((steps, slots, wide), BF16),
            pltpu.VMEM((n_slot, slots, wide), BF16),
            pltpu.VMEM((n_tok, 2, n_tp, rows, wide), BF16),
            pltpu.VMEM((n_slot, 2, n_tp, slots, wide), BF16),
            pltpu.VMEM((rows, wide), F32),
            dma((items + 3,)),
            dma((n_tp, 2)),
            dma((n_tp, 2)),
            dma((2, n_tp, items)),
            dma((n_tp, items)),
            dma((steps + n_slot,)),
            dma((steps + n_slot,)),
            dma((steps + n_slot,)),
            dma((steps + n_slot,)),
            dma((n_tp, items)),
            dma((2, n_tp, items)),
        ],
        compiler_params=pltpu.CompilerParams(
            collective_id=0, has_side_effects=True, vmem_limit_bytes=67043328
        ),
    )(
        tokens,
        norm_gain.astype(F32).reshape(1, width),
        expert_ids,
        gate_prob,
        w_gate[0],
        w_up[0],
        w_down[0],
    )


def solution(mesh):
    placed = (
        P("ep", "tp"),
        P("tp"),
        P("ep", None),
        P("ep", None),
        P("ep", None, "tp"),
        P("ep", None, "tp"),
        P("ep", "tp", None),
    )
    return jax.shard_map(
        local, mesh=mesh, in_specs=placed, out_specs=P("ep", "tp"), check_vma=False
    )
```

```python
import functools

import jax
import jax.numpy as jnp
from jax import lax
from jax.experimental import pallas as pl
from jax.experimental.pallas import tpu as pltpu
from jax.sharding import PartitionSpec as P

TOP = 8
EXP_DEV = 8
SHARE = 7
EPSILON = 1e-06
BF16 = jnp.bfloat16
F32 = jnp.float32


def look_up(table, index):
    span = len(table) ** 2
    total = 0
    for i, value in enumerate(table):
        if value:
            total = total + value * (1 - ((index - i) * (index - i) + span - 1) // span)
    return total


def near_first(n_tp):
    table = []
    for z in range(n_tp):
        inner = 1 if z < n_tp / 2 else -1
        table += sorted(range(n_tp), key=lambda s: (abs(s - z), -inner * (s - z)))
    return table


def body(
    n_ep, n_tp, rows, width, cap, wide, n_tok, n_slot,
    tok_hbm, gain_ref, ids_ref, prob_ref, gate_hbm, up_hbm, down_hbm,
    out_ref,
    tok, stats, rowscale, turned, slotscale, dmat, wmat, send, recv, slot_in, w_gate, w_up, w_down,
    acc, hid, ret, ret_slot, in_tok, in_slot, part,
    load_sem, st_send, st_recv, sc_send, sc_recv, zt_send, zt_recv, xs, xr, ys, yr, zp_send, zp_recv,
):
    e, z = lax.axis_index("ep"), lax.axis_index("tp")
    last = n_tp - 1
    items = n_tok + n_slot
    slots = n_ep * cap
    steps = n_tp * n_tok
    table = near_first(n_tp)

    def nth(k):
        return look_up(table, z * n_tp + k)

    def column(slice_index, item):
        return pl.multiple_of(slice_index * width + item * wide, wide)

    def remote(axis, index, src, dst, send_sem, recv_sem):
        return pltpu.make_async_remote_copy(
            src_ref=src,
            dst_ref=dst,
            send_sem=send_sem,
            recv_sem=recv_sem,
            device_id={axis: index},
            device_id_type=pl.DeviceIdType.MESH,
        )

    def each_peer(fn):
        def step(shift, carry):
            fn(lax.rem(e + shift, n_ep))
            return carry

        lax.fori_loop(1, n_ep, step, 0)

    loads = [
        pltpu.make_async_copy(
            tok_hbm.at[:, pl.ds(m * wide, wide)], tok.at[z, m], load_sem.at[m]
        )
        for m in range(items)
    ]
    weights = [
        pltpu.make_async_copy(src, dst, load_sem.at[items + i])
        for i, (src, dst) in enumerate(
            ((gate_hbm, w_gate), (up_hbm, w_up), (down_hbm, w_down))
        )
    ]
    for copy in loads + weights:
        copy.start()

    barrier = pltpu.get_barrier_semaphore()

    def greet(axis, index):
        pl.semaphore_signal(
            barrier, inc=1, device_id={axis: index}, device_id_type=pl.DeviceIdType.MESH
        )

    each_peer(lambda p: greet("ep", p))
    for shift in range(1, n_tp):
        greet("tp", lax.rem(z + shift, n_tp))

    ids = ids_ref[...].T
    prob = prob_ref[...].astype(F32).T
    lane = lax.broadcasted_iota(jnp.int32, (rows, 128), 1)
    picked = jnp.zeros((rows, 128), F32)
    chance = jnp.zeros((rows, 128), F32)
    for k in range(TOP):
        same = ids[:, k : k + 1] == lane
        picked = jnp.where(same, 1.0, picked)
        chance = jnp.where(same, prob[:, k : k + 1], chance)
    picked = picked.astype(BF16)
    earlier = (
        lax.broadcasted_iota(jnp.int32, (rows, rows), 1)
        < lax.broadcasted_iota(jnp.int32, (rows, rows), 0)
    )
    earlier = jnp.where(earlier, 1.0, 0.0).astype(BF16)
    before = jnp.dot(earlier, picked, preferred_element_type=F32).astype(BF16)
    spread_row = lax.broadcasted_iota(jnp.int32, (128, slots), 0)
    spread_col = lax.broadcasted_iota(jnp.int32, (128, slots), 1)
    spread = jnp.where(
        (spread_col >= spread_row * cap) & (spread_col < (spread_row + 1) * cap), 1.0, 0.0
    ).astype(BF16)
    is_picked = jnp.dot(picked, spread, preferred_element_type=F32)
    place = jnp.dot(before, spread, preferred_element_type=F32)
    weight = jnp.dot(chance.astype(BF16), spread, preferred_element_type=F32)
    position = lax.rem(lax.broadcasted_iota(jnp.int32, (rows, slots), 1), cap).astype(F32)
    hit = (is_picked > 0.5) & (place == position)
    wmat[...] = jnp.where(hit, weight, 0.0).astype(BF16)
    dmat[...] = jnp.where(hit, 1.0, 0.0).T.astype(BF16)

    pl.semaphore_wait(barrier, n_ep - 1 + n_tp - 1)

    def along(way, s, m, ref):
        peer = lax.rem(z + n_tp - 1 if way == 0 else z + 1, n_tp)
        return remote("tp", peer, ref, ref, zt_send.at[way, s, m], zt_recv.at[s, m])

    square = jnp.zeros((rows, wide), F32)
    gain = gain_ref[...].astype(F32).reshape(1, width)
    for m in range(items):
        loads[m].wait()
        values = tok[z, m].astype(F32)
        square = square + values * values
        tok[z, m] = (values * gain[:, m * wide : (m + 1) * wide]).astype(BF16)
        if m < n_tok:
            @pl.when(z > 0)
            def _():
                along(0, z, m, tok.at[z, m]).start()

            @pl.when(z < last)
            def _():
                along(1, z, m, tok.at[z, m]).start()

    square = jnp.sum(square, axis=1, keepdims=True)
    stats[z] = jnp.broadcast_to(square, (rows, 128)).T[0:8, :]

    def share(shift):
        peer = lax.rem(z + shift, n_tp)
        return remote("tp", peer, stats.at[z], stats.at[z], st_send.at[shift], st_recv.at[shift])

    for shift in range(1, n_tp):
        share(shift).start()

    def to_peers(index, dst, send_sem, recv_sem):
        own = pl.ds(pl.multiple_of(e * cap, cap), cap)
        dst[own, :] = send[index, own, :]

        def one(p):
            theirs = pl.ds(pl.multiple_of(p * cap, cap), cap)
            remote("ep", p, send.at[index, theirs, :], dst.at[own, :], send_sem, recv_sem).start()

        each_peer(one)

    def all_peers(index, dst, send_sem, recv_sem):
        most = pl.ds(0, (n_ep - 1) * cap)
        return remote(
            "ep", lax.rem(e + 1, n_ep), send.at[index, most, :], dst.at[most, :], send_sem, recv_sem
        )

    def dispatch(s, m, index, dst):
        placed = jnp.dot(dmat[...], tok[s, m], preferred_element_type=F32)
        send[index] = placed.astype(BF16)
        to_peers(index, dst, xs.at[index], xr.at[index])

    def gate_up(chunk, row, first=False):
        values = chunk[...]
        at = pl.ds(row, wide)
        for i, matrix in enumerate((w_gate, w_up)):
            product = jnp.dot(values, matrix[at, :], preferred_element_type=F32)
            acc[i] = product if first else acc[i] + product

    for a in range(n_slot):
        dispatch(z, n_tok + a, steps + a, slot_in.at[z, a])

    @pl.loop(0, n_tok)
    def _(j):
        dispatch(z, j, j, recv.at[j])

    weights[0].wait()
    weights[1].wait()
    for a in range(n_slot):
        all_peers(steps + a, slot_in.at[z, a], xs.at[steps + a], xr.at[steps + a]).wait_recv()

        @pl.when(z > 0)
        def _():
            along(0, z, n_tok + a, slot_in.at[z, a]).start()

        @pl.when(z < last)
        def _():
            along(1, z, n_tok + a, slot_in.at[z, a]).start()

        gate_up(slot_in.at[z, a], column(z, n_tok + a), first=a == 0)

    def scale_to(p):
        return remote("ep", p, rowscale.at[e], rowscale.at[e], sc_send.at[0], sc_recv.at[0])

    def all_scales():
        most = pl.ds(0, n_ep - 1)
        return remote(
            "ep", lax.rem(e + 1, n_ep), rowscale.at[most], rowscale.at[most], sc_send.at[0], sc_recv.at[0]
        )

    def send_scales():
        for shift in range(1, n_tp):
            share(shift).wait_recv()
        total = stats[0]
        for i in range(1, n_tp):
            total = total + stats[i]
        factor = lax.rsqrt(total / (width * n_tp) + EPSILON)
        by_slot = lax.dot_general(
            factor,
            dmat[...].astype(F32),
            (((1,), (1,)), ((), ())),
            precision=lax.Precision.HIGHEST,
            preferred_element_type=F32,
        )
        rowscale[e] = by_slot[0:1, :]
        each_peer(lambda p: scale_to(p).start())

    def turn_scales():
        all_scales().wait_recv()
        for block in range(n_ep):
            turned[...] = jnp.broadcast_to(rowscale[block], (8, slots)).T
            own = turned[pl.ds(pl.multiple_of(e * cap, cap), cap), 0:1]
            slotscale[block * cap : (block + 1) * cap, :] = jnp.broadcast_to(own, (cap, 128))

    def arrive(k, m, ref_of):
        @pl.when(z + k <= last)
        def _():
            along(0, z + k, m, ref_of(z + k)).wait_recv()

            @pl.when(z > 0)
            def _():
                along(0, z + k, m, ref_of(z + k)).start()

        @pl.when(z - k >= 0)
        def _():
            along(1, z - k, m, ref_of(z - k)).wait_recv()

            @pl.when(z < last)
            def _():
                along(1, z - k, m, ref_of(z - k)).start()

    def take_in(index, s, m):
        all_peers(index, recv.at[index], xs.at[index], xr.at[index]).wait_recv()
        gate_up(recv.at[index], column(s, m))

    @pl.loop(n_tok, steps)
    def _(i):
        k, j = i // n_tok, i % n_tok
        arrive(k, j, lambda s: tok.at[s, j])
        dispatch(nth(k), j, i, recv.at[i])
        take_in(i - n_tok, nth(k - 1), j)
        for a in range(n_slot):
            @pl.when((j == n_tok - 1) & (k < last))
            def _():
                arrive(k, n_tok + a, lambda s: slot_in.at[s, a])

        @pl.when(i == 2 * n_tok - 1)
        def _():
            send_scales()

    turn_scales()

    for a in range(n_slot):
        @pl.loop(1, last)
        def _(k):
            s = nth(k)
            gate_up(slot_in.at[s, a], column(s, n_tok + a))

    @pl.loop(0, n_tok)
    def _(j):
        take_in(steps - n_tok + j, nth(last), j)

    for a in range(n_slot):
        arrive(last, n_tok + a, lambda s: slot_in.at[s, a])
        s = nth(last)
        gate_up(slot_in.at[s, a], column(s, n_tok + a))

    gate_act = acc[0] * slotscale[:, 0:1]
    up_act = acc[1] * slotscale[:, 0:1]
    hid[...] = (gate_act / (1.0 + jnp.exp(-gate_act)) * up_act).astype(BF16)
    weights[2].wait()

    def down(index, s, m):
        matrix = w_down[:, pl.ds(column(s, m), wide)]
        send[index] = jnp.dot(hid[...], matrix, preferred_element_type=F32).astype(BF16)

    def onward(way, k, s, m, src, landing):
        peer = lax.rem(z + 1 if way == 0 else z + n_tp - 1, n_tp)
        return remote("tp", peer, src, landing.at[way, s], zp_send.at[k, m], zp_recv.at[way, s, m])

    for a in range(n_slot):
        all_peers(steps + a, slot_in.at[z, a], xs.at[steps + a], xr.at[steps + a]).wait_send()

    def far(k):
        return nth(last - k)

    def down_tok(i):
        all_peers(i, recv.at[i], xs.at[i], xr.at[i]).wait_send()
        down(i, far(i // n_tok), i % n_tok)
        to_peers(i, ret.at[i], ys.at[i], yr.at[i])

    @pl.loop(0, n_tok)
    def _(i):
        down_tok(i)

    for a in range(n_slot):
        @pl.loop(0, n_tp)
        def _(k):
            s, index = far(k), steps + k * n_slot + a
            down(index, s, n_tok + a)

            @pl.when((z == 0) & (k < last))
            def _():
                onward(0, k, s, n_tok + a, send.at[index], in_slot.at[a]).start()

            @pl.when((z == last) & (k < last))
            def _():
                onward(1, k, s, n_tok + a, send.at[index], in_slot.at[a]).start()

    @pl.loop(n_tok, steps)
    def _(i):
        down_tok(i)

    for a in range(n_slot):
        @pl.loop(0, last)
        def _(k):
            s, index = far(k), steps + k * n_slot + a

            def pass_on(way):
                copy = onward(way, k, s, n_tok + a, send.at[index], in_slot.at[a])
                copy.wait_recv()
                summed = send[index].astype(F32) + in_slot[a, way, s].astype(F32)
                send[index] = summed.astype(BF16)
                copy.start()

            @pl.when((s > z) & (z > 0))
            def _():
                pass_on(0)

            @pl.when((s < z) & (z < last))
            def _():
                pass_on(1)

    def combine(i):
        all_peers(i, ret.at[i], ys.at[i], yr.at[i]).wait_recv()
        return jnp.dot(wmat[...], ret[i], preferred_element_type=F32)

    def add_in(way, s, j):
        landing = in_tok.at[j]
        onward(way, 0, s, j, landing.at[way, s], landing).wait_recv()
        part[...] = part[...] + in_tok[j, way, s].astype(F32)

    def forward_part(i):
        k, j = i // n_tok, i % n_tok
        s = far(k)
        part[...] = combine(i)

        @pl.when((s > z) & (z > 0))
        def _():
            add_in(0, s, j)

        @pl.when((s < z) & (z < last))
        def _():
            add_in(1, s, j)

        recv[i, 0:rows, :] = part[...].astype(BF16)

        @pl.when(s > z)
        def _():
            onward(0, k, s, j, recv.at[i, pl.ds(0, rows), :], in_tok.at[j]).start()

        @pl.when(s < z)
        def _():
            onward(1, k, s, j, recv.at[i, pl.ds(0, rows), :], in_tok.at[j]).start()

    @pl.loop(0, n_tok)
    def _(i):
        forward_part(i)

    for a in range(n_slot):
        index = steps + last * n_slot + a

        def add_slot(way):
            copy = onward(way, 0, z, n_tok + a, send.at[index], in_slot.at[a])
            copy.wait_recv()
            send[index] = (send[index].astype(F32) + in_slot[a, way, z].astype(F32)).astype(BF16)

        @pl.when(z > 0)
        def _():
            add_slot(0)

        @pl.when(z < last)
        def _():
            add_slot(1)

        to_peers(index, ret_slot.at[a], ys.at[steps + a], yr.at[steps + a])

    @pl.loop(n_tok, steps - n_tok)
    def _(i):
        forward_part(i)

    @pl.loop(0, n_tok)
    def _(j):
        part[...] = combine(steps - n_tok + j)

        @pl.when(z > 0)
        def _():
            add_in(0, z, j)

        @pl.when(z < last)
        def _():
            add_in(1, z, j)

        out_ref[:, pl.ds(pl.multiple_of(j * wide, wide), wide)] = part[...].astype(BF16)

    for a in range(n_slot):
        index = steps + last * n_slot + a
        all_peers(index, ret_slot.at[a], ys.at[steps + a], yr.at[steps + a]).wait_recv()
        m = n_tok + a
        out_ref[:, m * wide : (m + 1) * wide] = jnp.dot(
            wmat[...], ret_slot[a], preferred_element_type=F32
        ).astype(BF16)

    all_scales().wait_send()
    for shift in range(1, n_tp):
        share(shift).wait_send()

    @pl.loop(0, n_tp)
    def _(s):
        @pl.when((z > 0) & (s >= z))
        def _():
            for m in range(items):
                ref = tok.at[s, m] if m < n_tok else slot_in.at[s, m - n_tok]
                along(0, s, m, ref).wait_send()

        @pl.when((z < last) & (s <= z))
        def _():
            for m in range(items):
                ref = tok.at[s, m] if m < n_tok else slot_in.at[s, m - n_tok]
                along(1, s, m, ref).wait_send()

    @pl.loop(0, steps)
    def _(i):
        all_peers(i, ret.at[i], ys.at[i], yr.at[i]).wait_send()

    for a in range(n_slot):
        index = steps + last * n_slot + a
        all_peers(index, ret_slot.at[a], ys.at[steps + a], yr.at[steps + a]).wait_send()

    @pl.loop(0, last)
    def _(k):
        for m in range(n_tok):
            onward(
                0, k, 0, m, recv.at[k * n_tok + m, pl.ds(0, rows), :], in_tok.at[m]
            ).wait_send()
        for a in range(n_slot):
            onward(
                0, k, 0, n_tok + a, send.at[steps + k * n_slot + a], in_slot.at[a]
            ).wait_send()


def local(tokens, norm_gain, expert_ids, gate_prob, w_gate, w_up, w_down):
    n_ep = lax.axis_size("ep")
    n_tp = lax.axis_size("tp")
    rows, width = tokens.shape
    cap = max(2, 2 * rows * TOP // (EXP_DEV * n_ep))
    slots = n_ep * cap
    wide = 256 if width % 256 == 0 else 128
    items = width // wide
    n_slot = max(1, items // SHARE)
    n_tok = items - n_slot
    units = w_gate.shape[2]
    steps = n_tp * n_tok

    kernel = functools.partial(body, n_ep, n_tp, rows, width, cap, wide, n_tok, n_slot)
    vmem = pl.BlockSpec(memory_space=pltpu.VMEM)
    hbm = pl.BlockSpec(memory_space=pl.ANY)
    dma = pltpu.SemaphoreType.DMA
    return pl.pallas_call(
        kernel,
        out_shape=jax.ShapeDtypeStruct((rows, width), BF16),
        in_specs=[hbm, vmem, vmem, vmem, hbm, hbm, hbm],
        out_specs=vmem,
        scratch_shapes=[
            pltpu.VMEM((n_tp, items, rows, wide), BF16),
            pltpu.VMEM((n_tp, 8, rows), F32),
            pltpu.VMEM((n_ep, 1, slots), F32),
            pltpu.VMEM((slots, 8), F32),
            pltpu.VMEM((slots, 128), F32),
            pltpu.VMEM((slots, rows), BF16),
            pltpu.VMEM((rows, slots), BF16),
            pltpu.VMEM((n_tp * items, slots, wide), BF16),
            pltpu.VMEM((steps, slots, wide), BF16),
            pltpu.VMEM((n_tp, n_slot, slots, wide), BF16),
            pltpu.VMEM((n_tp * width, units), BF16),
            pltpu.VMEM((n_tp * width, units), BF16),
            pltpu.VMEM((units, n_tp * width), BF16),
            pltpu.VMEM((2, slots, units), F32),
            pltpu.VMEM((slots, units), BF16),
            pltpu.VMEM((steps, slots, wide), BF16),
            pltpu.VMEM((n_slot, slots, wide), BF16),
            pltpu.VMEM((n_tok, 2, n_tp, rows, wide), BF16),
            pltpu.VMEM((n_slot, 2, n_tp, slots, wide), BF16),
            pltpu.VMEM((rows, wide), F32),
            dma((items + 3,)),
            dma((n_tp,)),
            dma((n_tp,)),
            dma((1,)),
            dma((1,)),
            dma((2, n_tp, items)),
            dma((n_tp, items)),
            dma((steps + n_slot,)),
            dma((steps + n_slot,)),
            dma((steps + n_slot,)),
            dma((steps + n_slot,)),
            dma((n_tp, items)),
            dma((2, n_tp, items)),
        ],
        compiler_params=pltpu.CompilerParams(
            collective_id=0, has_side_effects=True, vmem_limit_bytes=67043328
        ),
    )(
        tokens,
        norm_gain,
        expert_ids.T,
        gate_prob.T,
        w_gate[0],
        w_up[0],
        w_down[0],
    )


def solution(mesh):
    placed = (
        P("ep", "tp"),
        P("tp"),
        P("ep", None),
        P("ep", None),
        P("ep", None, "tp"),
        P("ep", None, "tp"),
        P("ep", "tp", None),
    )
    return jax.shard_map(
        local, mesh=mesh, in_specs=placed, out_specs=P("ep", "tp"), check_vma=False
    )
```

```python
import functools

import jax
import jax.numpy as jnp
from jax import lax
from jax.experimental import pallas as pl
from jax.experimental.pallas import tpu as pltpu
from jax.sharding import PartitionSpec as P

TOP = 8
EXP_DEV = 8
SHARES = ((1, 3), (3, 1))
PARTS = 7
UNROLL = 8
EPSILON = 1e-06
BF16 = jnp.bfloat16
F32 = jnp.float32


def look_up(table, index):
    span = len(table) ** 2
    total = 0
    for i, value in enumerate(table):
        if value:
            total = total + value * (1 - ((index - i) * (index - i) + span - 1) // span)
    return total


def near_first(n_tp):
    table = []
    for z in range(n_tp):
        inner = 1 if z < n_tp / 2 else -1
        table += sorted(range(n_tp), key=lambda s: (abs(s - z), -inner * (s - z)))
    return table


class Half:
    def __init__(self, core, items):
        forth, back = (max(1, items * share // PARTS) for share in SHARES[core])
        self.core = core
        self.d_slot, self.d_tok = forth, items - forth
        self.r_slot, self.r_tok = back, items - back


def buffers(n_ep, n_tp, rows, width, cap, wide, units, halves):
    items = width // wide
    slots, some = n_ep * cap, n_ep // 2 * cap
    most_d = max(n_tp * half.d_tok + half.d_slot for half in halves)
    most_r = max(n_tp * half.r_tok + half.r_slot for half in halves)
    most_tok = max(half.r_tok for half in halves)
    dma = pltpu.SemaphoreType.DMA
    names = dict(
        tok=pltpu.VMEM((n_tp, items, rows, wide), BF16),
        stats=pltpu.VMEM((n_tp, 8, rows), F32),
        rowscale=pltpu.VMEM((n_ep, 1, slots), F32),
        turned=pltpu.VMEM((slots, 8), F32),
        slotscale=pltpu.VMEM((2, some, 128), F32),
        dmat=pltpu.VMEM((slots, rows), BF16),
        wmat=pltpu.VMEM((rows, slots), BF16),
        send=pltpu.VMEM((most_d, slots, wide), BF16),
        w_gate=pltpu.VMEM((n_tp * width, units), BF16),
        w_up=pltpu.VMEM((n_tp * width, units), BF16),
        w_down=pltpu.VMEM((units, n_tp * width), BF16),
        ret=pltpu.VMEM((most_r, slots, wide), BF16),
        in_tok=pltpu.VMEM((most_tok, n_tp + 1, rows, wide), BF16),
        part=pltpu.VMEM((rows, wide), F32),
        load_sem=dma((items + 3,)),
        st_send=dma((n_tp,)),
        st_recv=dma((n_tp,)),
        sc_send=dma((1,)),
        sc_recv=dma((1,)),
        zt_send=dma((2, n_tp, items)),
        zt_recv=dma((n_tp, items)),
        xs=dma((most_d,)),
        yr=dma((most_r,)),
        pt_send=dma((n_tp, items)),
        pt_recv=dma((2, n_tp, items)),
    )
    for half in halves:
        h = half.core
        names.update({
            f"recv{h}": pltpu.VMEM((n_tp * half.d_tok, some, wide), BF16),
            f"slot_in{h}": pltpu.VMEM((n_tp, half.d_slot, some, wide), BF16),
            f"acc{h}": pltpu.VMEM((2, some, units), F32),
            f"hid{h}": pltpu.VMEM((some, units), BF16),
            f"ysend{h}": pltpu.VMEM((n_tp * items, some, wide), BF16),
            f"in_slot{h}": pltpu.VMEM((half.r_slot, n_tp + 1, some, wide), BF16),
            f"zs_send{h}": dma((2, n_tp, half.d_slot)),
            f"zs_recv{h}": dma((n_tp, half.d_slot)),
            f"xr{h}": dma((n_tp * half.d_tok + half.d_slot,)),
            f"ys{h}": dma((n_tp * half.r_tok + half.r_slot,)),
            f"ps_send{h}": dma((n_tp, half.r_slot)),
            f"ps_recv{h}": dma((2, n_tp, half.r_slot)),
        })
    return names


def body(names, halves, n_ep, n_tp, rows, width, cap, wide, *refs):
    tok_hbm, gain_ref, ids_ref, prob_ref, gate_hbm, up_hbm, down_hbm, out_ref = refs[:8]
    r = dict(zip(names, refs[8:]))
    tok, send, ret, in_tok, part = (r[n] for n in ("tok", "send", "ret", "in_tok", "part"))
    w_gate, w_up, w_down = r["w_gate"], r["w_up"], r["w_down"]
    dmat, wmat, stats, rowscale = r["dmat"], r["wmat"], r["stats"], r["rowscale"]
    e, z = lax.axis_index("ep"), lax.axis_index("tp")
    core, seat = lax.rem(e, 2), e // 2
    last = n_tp - 1
    items = width // wide
    slots, n_src = n_ep * cap, n_ep // 2
    table = near_first(n_tp)

    def nth(k):
        return look_up(table, z * n_tp + k)

    def far(k):
        return nth(last - k)

    def column(s, m):
        return pl.multiple_of(s * width + m * wide, wide)

    def block(i):
        return pl.ds(pl.multiple_of(i * cap, cap), cap)

    def mine(half):
        return core == half.core

    def remote(axis, index, src, dst, send_sem, recv_sem):
        return pltpu.make_async_remote_copy(
            src_ref=src,
            dst_ref=dst,
            send_sem=send_sem,
            recv_sem=recv_sem,
            device_id={axis: index},
            device_id_type=pl.DeviceIdType.MESH,
        )

    def awaited(ref, count, send_sem, recv_sem):
        some = ref.at[pl.ds(0, count)]
        return remote("ep", lax.rem(e + 1, n_ep), some, some, send_sem, recv_sem)

    def repeat(first, past, fn):
        if past <= UNROLL:
            for i in range(first, past):
                fn(i)
        else:
            pl.loop(first, past)(fn)

    def each_peer(fn):
        repeat(1, n_ep, lambda shift: fn(lax.rem(e + shift, n_ep)))

    def next_to(way):
        return lax.rem(z + n_tp - 1 if way == 0 else z + 1, n_tp)

    loads = [
        pltpu.make_async_copy(
            tok_hbm.at[:, pl.ds(m * wide, wide)], tok.at[z, m], r["load_sem"].at[m]
        )
        for m in range(items)
    ]
    weights = [
        pltpu.make_async_copy(src, dst, r["load_sem"].at[items + i])
        for i, (src, dst) in enumerate(
            ((gate_hbm, w_gate), (up_hbm, w_up), (down_hbm, w_down))
        )
    ]
    for copy in loads + weights:
        copy.start()

    barrier = pltpu.get_barrier_semaphore()

    def greet(axis, index):
        pl.semaphore_signal(
            barrier, inc=1, device_id={axis: index}, device_id_type=pl.DeviceIdType.MESH
        )

    each_peer(lambda p: greet("ep", p))
    for shift in range(1, n_tp):
        greet("tp", lax.rem(z + shift, n_tp))

    ids = ids_ref[...].T
    prob = prob_ref[...].astype(F32).T
    lane = lax.broadcasted_iota(jnp.int32, (rows, 128), 1)
    picked = jnp.zeros((rows, 128), F32)
    chance = jnp.zeros((rows, 128), F32)
    for k in range(TOP):
        same = ids[:, k : k + 1] == lane
        picked = jnp.where(same, 1.0, picked)
        chance = jnp.where(same, prob[:, k : k + 1], chance)
    picked = picked.astype(BF16)
    earlier = (
        lax.broadcasted_iota(jnp.int32, (rows, rows), 1)
        < lax.broadcasted_iota(jnp.int32, (rows, rows), 0)
    )
    earlier = jnp.where(earlier, 1.0, 0.0).astype(BF16)
    before = jnp.dot(earlier, picked, preferred_element_type=F32).astype(BF16)
    spread_row = lax.broadcasted_iota(jnp.int32, (128, slots), 0)
    spread_col = lax.broadcasted_iota(jnp.int32, (128, slots), 1)
    spread = jnp.where(
        (spread_col >= spread_row * cap) & (spread_col < (spread_row + 1) * cap), 1.0, 0.0
    ).astype(BF16)
    is_picked = jnp.dot(picked, spread, preferred_element_type=F32)
    place = jnp.dot(before, spread, preferred_element_type=F32)
    weight = jnp.dot(chance.astype(BF16), spread, preferred_element_type=F32)
    position = lax.rem(lax.broadcasted_iota(jnp.int32, (rows, slots), 1), cap).astype(F32)
    hit = (is_picked > 0.5) & (place == position)
    wmat[...] = jnp.where(hit, weight, 0.0).astype(BF16)
    dmat[...] = jnp.where(hit, 1.0, 0.0).T.astype(BF16)

    pl.semaphore_wait(barrier, n_ep - 1 + n_tp - 1)

    def along(way, s, m):
        return remote(
            "tp", next_to(way), tok.at[s, m], tok.at[s, m],
            r["zt_send"].at[way, s, m], r["zt_recv"].at[s, m],
        )

    def along_slot(half, way, s, a):
        h = half.core
        ref = r[f"slot_in{h}"].at[s, a]
        return remote(
            "tp", next_to(way), ref, ref,
            r[f"zs_send{h}"].at[way, s, a], r[f"zs_recv{h}"].at[s, a],
        )

    def both_ways(copy):
        @pl.when(z > 0)
        def _():
            copy(0).start()

        @pl.when(z < last)
        def _():
            copy(1).start()

    square = jnp.zeros((rows, wide), F32)
    gain = gain_ref[...].astype(F32).reshape(1, width)
    for m in range(items):
        loads[m].wait()
        values = tok[z, m].astype(F32)
        square = square + values * values
        tok[z, m] = (values * gain[:, m * wide : (m + 1) * wide]).astype(BF16)
        if m < halves[0].d_tok:
            @pl.when(mine(halves[0]))
            def _():
                both_ways(lambda way: along(way, z, m))

    square = jnp.sum(square, axis=1, keepdims=True)
    stats[z] = jnp.broadcast_to(square, (rows, 128)).T[0:8, :]

    def share(shift):
        ref = stats.at[z]
        peer = lax.rem(z + shift, n_tp)
        return remote("tp", peer, ref, ref, r["st_send"].at[shift], r["st_recv"].at[shift])

    for shift in range(1, n_tp):
        share(shift).start()

    def dispatch(half, s, m, index, dst):
        placed = jnp.dot(dmat[...], tok[s, m], preferred_element_type=F32)
        send[index] = placed.astype(BF16)
        dst[block(seat), :] = send[index, block(e), :]
        sems = r["xs"].at[index], r[f"xr{half.core}"].at[index]
        each_peer(
            lambda p: remote("ep", p, send.at[index, block(p)], dst.at[block(seat)], *sems).start()
        )

    def wait_in(half, index, dst):
        sems = r["xs"].at[index], r[f"xr{half.core}"].at[index]

        @pl.when(mine(half))
        def _():
            awaited(dst, (n_src - 1) * cap, *sems).wait_recv()

        @pl.when(core != half.core)
        def _():
            awaited(dst, n_src * cap, *sems).wait_recv()

    def wait_out(half):
        @pl.when(mine(half))
        def _():
            @pl.loop(0, n_tp * half.d_tok + half.d_slot)
            def _(i):
                sem = r["xs"].at[i]
                awaited(send.at[i], (n_ep - 1) * cap, sem, sem).wait_send()

    def gate_up(half, chunk, row, first=False):
        acc = r[f"acc{half.core}"]
        values = chunk[...]
        at = pl.ds(row, wide)
        for i, matrix in enumerate((w_gate, w_up)):
            product = jnp.dot(values, matrix[at, :], preferred_element_type=F32)
            acc[i] = product if first else acc[i] + product

    def slot_ref(half):
        slot_in = r[f"slot_in{half.core}"]
        return lambda s, a: slot_in.at[s, a]

    def own_slots_out(half):
        @pl.when(mine(half))
        def _():
            for a in range(half.d_slot):
                index = n_tp * half.d_tok + a
                dispatch(half, z, half.d_tok + a, index, slot_ref(half)(z, a))

    def own_toks_out(half):
        @pl.when(mine(half))
        def _():
            @pl.loop(0, half.d_tok)
            def _(j):
                dispatch(half, z, j, j, r[f"recv{half.core}"].at[j])

    def own_slots_in(half):
        for a in range(half.d_slot):
            ref = slot_ref(half)(z, a)
            wait_in(half, n_tp * half.d_tok + a, ref)
            both_ways(lambda way: along_slot(half, way, z, a))

    def own_slots_used(half):
        for a in range(half.d_slot):
            gate_up(half, slot_ref(half)(z, a), column(z, half.d_tok + a), first=a == 0)

    def arrive(k, copy):
        @pl.when(z + k <= last)
        def _():
            copy(0, z + k).wait_recv()

            @pl.when(z > 0)
            def _():
                copy(0, z + k).start()

        @pl.when(z - k >= 0)
        def _():
            copy(1, z - k).wait_recv()

            @pl.when(z < last)
            def _():
                copy(1, z - k).start()

    def tok_on(half, k, j):
        @pl.when(mine(half))
        def _():
            arrive(k, lambda way, s: along(way, s, j))
            index = k * half.d_tok + j
            dispatch(half, nth(k), j, index, r[f"recv{half.core}"].at[index])

    def slots_on(half, k):
        for a in range(half.d_slot):
            arrive(k, lambda way, s: along_slot(half, way, s, a))

    def slots_used(half, k):
        s = nth(k)
        for a in range(half.d_slot):
            gate_up(half, slot_ref(half)(s, a), column(s, half.d_tok + a))

    def take_in(half, k, j):
        index = k * half.d_tok + j
        ref = r[f"recv{half.core}"].at[index]
        wait_in(half, index, ref)
        gate_up(half, ref, column(nth(k), j))

    def take_in_all(half, first, past):
        @pl.loop(first * half.d_tok, past * half.d_tok)
        def _(i):
            take_in(half, i // half.d_tok, lax.rem(i, half.d_tok))

    def hidden(half):
        h = half.core
        scale = r["slotscale"][h, :, 0:1]
        gate_act = r[f"acc{h}"][0] * scale
        up_act = r[f"acc{h}"][1] * scale
        r[f"hid{h}"][...] = (gate_act / (1.0 + jnp.exp(-gate_act)) * up_act).astype(BF16)

    def scale_to(p):
        ref = rowscale.at[e]
        return remote("ep", p, ref, ref, r["sc_send"].at[0], r["sc_recv"].at[0])

    def all_scales():
        return awaited(rowscale, n_ep - 1, r["sc_send"].at[0], r["sc_recv"].at[0])

    def send_scales():
        for shift in range(1, n_tp):
            share(shift).wait_recv()
        total = stats[0]
        for i in range(1, n_tp):
            total = total + stats[i]
        factor = lax.rsqrt(total / (width * n_tp) + EPSILON)
        by_slot = lax.dot_general(
            factor,
            dmat[...].astype(F32),
            (((1,), (1,)), ((), ())),
            precision=lax.Precision.HIGHEST,
            preferred_element_type=F32,
        )
        rowscale[e] = by_slot[0:1, :]
        each_peer(lambda p: scale_to(p).start())

    def turn_scales():
        all_scales().wait_recv()
        for source in range(n_ep):
            r["turned"][...] = jnp.broadcast_to(rowscale[source], (8, slots)).T
            own = r["turned"][block(e), 0:1]
            at = source // 2 * cap
            r["slotscale"][source % 2, at : at + cap, :] = jnp.broadcast_to(own, (cap, 128))

    def down(half, index, s, m):
        matrix = w_down[:, pl.ds(column(s, m), wide)]
        h = half.core
        r[f"ysend{h}"][index] = jnp.dot(
            r[f"hid{h}"][...], matrix, preferred_element_type=F32
        ).astype(BF16)

    def to_owners(half, index, slot):
        ysend = r[f"ysend{half.core}"]
        sems = r[f"ys{half.core}"].at[slot], r["yr"].at[slot]

        def to_seat(shift):
            q = lax.rem(seat + shift, n_src)
            remote(
                "ep", 2 * q + half.core, ysend.at[index, block(q)], ret.at[slot, block(e)], *sems
            ).start()

        @pl.when(mine(half))
        def _():
            ret[slot, block(e), :] = ysend[index, block(seat), :]

        @pl.when(core != half.core)
        def _():
            to_seat(0)

        repeat(1, n_src, to_seat)

    def sent_to_owners(half, slot):
        sem = r[f"ys{half.core}"].at[slot]
        ref = r[f"ysend{half.core}"].at[0]

        @pl.when(mine(half))
        def _():
            awaited(ref, (n_src - 1) * cap, sem, sem).wait_send()

        @pl.when(core != half.core)
        def _():
            awaited(ref, n_src * cap, sem, sem).wait_send()

    def seat_of(way, s):
        if way == 0:
            return s
        return s + (n_tp - s) * (1 - (z - 1 - s + n_tp - 1) // n_tp)

    def onward(way, k, s, m, src):
        return remote(
            "tp", next_to(1 - way), src, in_tok.at[m, seat_of(way, s)],
            r["pt_send"].at[k, m], r["pt_recv"].at[way, s, m],
        )

    def onward_slot(half, way, k, s, a, src):
        h = half.core
        return remote(
            "tp", next_to(1 - way), src, r[f"in_slot{h}"].at[a, seat_of(way, s)],
            r[f"ps_send{h}"].at[k, a], r[f"ps_recv{h}"].at[way, s, a],
        )

    def slot_index(half, k, a):
        return n_tp * half.r_tok + k * half.r_slot + a

    def toks_down(half, first, past):
        @pl.loop(first * half.r_tok, past * half.r_tok)
        def _(i):
            down(half, i, far(i // half.r_tok), lax.rem(i, half.r_tok))
            to_owners(half, i, i)

    def slots_down(half, first, past):
        @pl.loop(first, past)
        def _(k):
            for a in range(half.r_slot):
                s, index = far(k), slot_index(half, k, a)
                down(half, index, s, half.r_tok + a)
                ref = r[f"ysend{half.core}"].at[index]

                @pl.when((z == 0) & (k < last))
                def _():
                    onward_slot(half, 0, k, s, a, ref).start()

                @pl.when((z == last) & (k < last))
                def _():
                    onward_slot(half, 1, k, s, a, ref).start()

    def slots_pass(half, k):
        ysend, in_slot = r[f"ysend{half.core}"], r[f"in_slot{half.core}"]
        s = far(k)
        for a in range(half.r_slot):
            index = slot_index(half, k, a)

            def pass_on(way):
                copy = onward_slot(half, way, k, s, a, ysend.at[index])
                awaited_here = remote(
                    "tp", next_to(way), in_slot.at[a, s], in_slot.at[a, s],
                    r[f"ps_send{half.core}"].at[k, a], r[f"ps_recv{half.core}"].at[way, s, a],
                )
                awaited_here.wait_recv()
                summed = ysend[index].astype(F32) + in_slot[a, s].astype(F32)
                ysend[index] = summed.astype(BF16)
                copy.start()

            @pl.when((s > z) & (z > 0))
            def _():
                pass_on(0)

            @pl.when((s < z) & (z < last))
            def _():
                pass_on(1)

    def own_slots_back(half):
        ysend, in_slot = r[f"ysend{half.core}"], r[f"in_slot{half.core}"]
        for a in range(half.r_slot):
            index = slot_index(half, last, a)

            def add(way, at):
                ref = in_slot.at[a, at]
                remote(
                    "tp", next_to(way), ref, ref,
                    r[f"ps_send{half.core}"].at[0, a], r[f"ps_recv{half.core}"].at[way, z, a],
                ).wait_recv()
                summed = ysend[index].astype(F32) + in_slot[a, at].astype(F32)
                ysend[index] = summed.astype(BF16)

            @pl.when(z > 0)
            def _():
                add(0, z)

            @pl.when(z < last)
            def _():
                add(1, n_tp)

            to_owners(half, index, n_tp * half.r_tok + a)

    def combine(i):
        sem = r["yr"].at[i]
        awaited(ret.at[i], (n_ep - 1) * cap, sem, sem).wait_recv()
        return jnp.dot(wmat[...], ret[i], preferred_element_type=F32)

    def add_in(way, s, at, j):
        ref = in_tok.at[j, at]
        remote(
            "tp", next_to(way), ref, ref, r["pt_send"].at[0, j], r["pt_recv"].at[way, s, j]
        ).wait_recv()
        part[...] = part[...] + in_tok[j, at].astype(F32)

    def parts_on(half, first, past, where=True):
        @pl.when(mine(half) & where)
        def _():
            @pl.loop(first * half.r_tok, past * half.r_tok)
            def _(i):
                k, j = i // half.r_tok, lax.rem(i, half.r_tok)
                s = far(k)
                part[...] = combine(i)

                @pl.when((s > z) & (z > 0))
                def _():
                    add_in(0, s, s, j)

                @pl.when((s < z) & (z < last))
                def _():
                    add_in(1, s, s, j)

                send[i, 0:rows, :] = part[...].astype(BF16)
                ref = send.at[i, pl.ds(0, rows)]

                @pl.when(s > z)
                def _():
                    onward(0, k, s, j, ref).start()

                @pl.when(s < z)
                def _():
                    onward(1, k, s, j, ref).start()

    def finish(half):
        @pl.when(mine(half))
        def _():
            @pl.loop(0, half.r_tok)
            def _(j):
                part[...] = combine(last * half.r_tok + j)

                @pl.when(z > 0)
                def _():
                    add_in(0, z, z, j)

                @pl.when(z < last)
                def _():
                    add_in(1, z, n_tp, j)

                out_ref[:, pl.ds(pl.multiple_of(j * wide, wide), wide)] = part[...].astype(BF16)

            for a in range(half.r_slot):
                m = half.r_tok + a
                out_ref[:, m * wide : (m + 1) * wide] = combine(n_tp * half.r_tok + a).astype(BF16)

    one, two = halves
    at_end = (z == 0) | (z == last)
    inside = (z > 0) & (z < last)

    own_slots_out(one)
    own_toks_out(one)
    weights[0].wait()
    weights[1].wait()
    own_slots_in(one)
    own_slots_used(one)

    @pl.loop(one.d_tok, n_tp * one.d_tok)
    def _(i):
        k, j = i // one.d_tok, lax.rem(i, one.d_tok)
        tok_on(one, k, j)
        take_in(one, k - 1, j)

        @pl.when((j == one.d_tok - 1) & (k < last))
        def _():
            slots_on(one, k)

        @pl.when(i == 2 * one.d_tok - 1)
        def _():
            send_scales()

    @pl.when(mine(two))
    def _():
        for m in range(two.d_tok):
            both_ways(lambda way: along(way, z, m))

    own_slots_out(two)
    turn_scales()

    @pl.loop(1, last)
    def _(k):
        slots_used(one, k)

    take_in_all(one, last, n_tp)
    own_toks_out(two)
    slots_on(one, last)
    slots_used(one, last)
    own_slots_in(two)
    hidden(one)
    weights[2].wait()
    wait_out(one)

    def toks_on(half, k):
        @pl.loop(0, half.d_tok)
        def _(j):
            tok_on(half, k, j)

    slots_down(one, 0, 1)
    toks_down(one, 0, 1)
    toks_on(two, 1)
    slots_down(one, 1, n_tp)
    toks_down(one, 1, n_tp)
    own_slots_used(two)
    slots_on(two, 1)
    for k in range(2, last):
        slots_pass(one, k - 2)
        toks_on(two, k)
        parts_on(one, k - 2, k - 1, at_end)
        slots_pass(one, k - 1)
        if k < last - 1:
            slots_on(two, k)
    slots_pass(one, last - 1)
    toks_on(two, last)
    parts_on(one, last - 2, last, at_end)
    slots_on(two, last - 1)
    own_slots_back(one)
    parts_on(one, 0, 1, inside)
    take_in_all(two, 0, 1)
    parts_on(one, 1, last - 1, inside)
    take_in_all(two, 1, last)
    parts_on(one, last - 1, last, inside)

    @pl.loop(1, last)
    def _(k):
        slots_used(two, k)

    take_in_all(two, last, n_tp)
    slots_on(two, last)
    slots_used(two, last)
    hidden(two)
    wait_out(two)

    toks_down(two, 0, 1)
    slots_down(two, 0, n_tp)
    toks_down(two, 1, n_tp)
    finish(one)
    for k in range(last):
        slots_pass(two, k)
    parts_on(two, 0, 1)
    own_slots_back(two)
    parts_on(two, 1, last)
    finish(two)

    all_scales().wait_send()
    for shift in range(1, n_tp):
        share(shift).wait_send()

    for half in halves:
        @pl.loop(0, n_tp)
        def _(s):
            for way, sends in enumerate(((z > 0) & (s >= z), (z < last) & (s <= z))):
                @pl.when(sends)
                def _():
                    for a in range(half.d_slot):
                        along_slot(half, way, s, a).wait_send()

                    @pl.when(mine(half))
                    def _():
                        for m in range(half.d_tok):
                            along(way, s, m).wait_send()

        @pl.loop(0, n_tp * half.r_tok + half.r_slot)
        def _(i):
            sent_to_owners(half, i)

        @pl.loop(0, last)
        def _(k):
            for a in range(half.r_slot):
                onward_slot(half, 0, k, 0, a, r[f"ysend{half.core}"].at[0]).wait_send()

            @pl.when(mine(half))
            def _():
                for m in range(half.r_tok):
                    onward(0, k, 0, m, send.at[0, pl.ds(0, rows)]).wait_send()


def local(tokens, norm_gain, expert_ids, gate_prob, w_gate, w_up, w_down):
    n_ep = lax.axis_size("ep")
    n_tp = lax.axis_size("tp")
    rows, width = tokens.shape
    cap = max(2, 2 * rows * TOP // (EXP_DEV * n_ep))
    wide = 256 if width % 256 == 0 else 128
    halves = [Half(core, width // wide) for core in range(2)]
    names = buffers(n_ep, n_tp, rows, width, cap, wide, w_gate.shape[2], halves)
    kernel = functools.partial(
        body, list(names), halves, n_ep, n_tp, rows, width, cap, wide
    )
    vmem = pl.BlockSpec(memory_space=pltpu.VMEM)
    hbm = pl.BlockSpec(memory_space=pl.ANY)
    return pl.pallas_call(
        kernel,
        out_shape=jax.ShapeDtypeStruct((rows, width), BF16),
        in_specs=[hbm, vmem, vmem, vmem, hbm, hbm, hbm],
        out_specs=vmem,
        scratch_shapes=list(names.values()),
        compiler_params=pltpu.CompilerParams(
            collective_id=0, has_side_effects=True, vmem_limit_bytes=67043328
        ),
        name="moe",
    )(
        tokens,
        norm_gain,
        expert_ids.T,
        gate_prob.T,
        w_gate[0],
        w_up[0],
        w_down[0],
    )


def solution(mesh):
    placed = (
        P("ep", "tp"),
        P("tp"),
        P("ep", None),
        P("ep", None),
        P("ep", None, "tp"),
        P("ep", None, "tp"),
        P("ep", "tp", None),
    )
    return jax.shard_map(
        local, mesh=mesh, in_specs=placed, out_specs=P("ep", "tp"), check_vma=False
    )
```

```python
import functools

import jax
import jax.numpy as jnp
from jax import lax
from jax.experimental import pallas as pl
from jax.experimental.pallas import tpu as pltpu
from jax.sharding import PartitionSpec as P

TOP = 8
EXP_DEV = 8
SHARES = ((1, 3), (3, 1))
PARTS = 7
UNROLL = 8
EPSILON = 1e-06
BF16 = jnp.bfloat16
F32 = jnp.float32


def look_up(table, index):
    span = len(table) ** 2
    total = 0
    for i, value in enumerate(table):
        if value:
            total = total + value * (1 - ((index - i) * (index - i) + span - 1) // span)
    return total


def near_first(n_tp):
    table = []
    for z in range(n_tp):
        inner = 1 if z < n_tp / 2 else -1
        table += sorted(range(n_tp), key=lambda s: (abs(s - z), -inner * (s - z)))
    return table


class Half:
    def __init__(self, core, items):
        forth, back = (max(1, items * share // PARTS) for share in SHARES[core])
        self.core = core
        self.d_slot, self.d_tok = forth, items - forth
        self.r_slot, self.r_tok = back, items - back


def buffers(n_ep, n_tp, rows, width, cap, wide, units, halves):
    items = width // wide
    slots, some = n_ep * cap, n_ep // 2 * cap
    most_d = max(n_tp * half.d_tok + half.d_slot for half in halves)
    most_r = max(n_tp * half.r_tok + half.r_slot for half in halves)
    most_tok = max(half.r_tok for half in halves)
    dma = pltpu.SemaphoreType.DMA
    names = dict(
        tok=pltpu.VMEM((n_tp, items, rows, wide), BF16),
        stats=pltpu.VMEM((n_tp, 8, rows), F32),
        rowscale=pltpu.VMEM((n_ep, 1, slots), F32),
        turned=pltpu.VMEM((slots, 8), F32),
        slotscale=pltpu.VMEM((2, some, 128), F32),
        dmat=pltpu.VMEM((slots, rows), BF16),
        wmat=pltpu.VMEM((rows, slots), BF16),
        send=pltpu.VMEM((most_d, slots, wide), BF16),
        w_gate=pltpu.VMEM((n_tp * width, units), BF16),
        w_up=pltpu.VMEM((n_tp * width, units), BF16),
        w_down=pltpu.VMEM((units, n_tp * width), BF16),
        ret=pltpu.VMEM((most_r, slots, wide), BF16),
        in_tok=pltpu.VMEM((most_tok, n_tp + 1, rows, wide), BF16),
        part=pltpu.VMEM((rows, wide), F32),
        result=pltpu.VMEM((items, rows, wide), BF16),
        load_sem=dma((items + 3,)),
        out_sem=dma((items,)),
        st_send=dma((n_tp,)),
        st_recv=dma((n_tp,)),
        sc_send=dma((1,)),
        sc_recv=dma((1,)),
        zt_send=dma((2, n_tp, items)),
        zt_recv=dma((n_tp, items)),
        xs=dma((most_d,)),
        yr=dma((most_r,)),
        pt_send=dma((n_tp, items)),
        pt_recv=dma((2, n_tp, items)),
    )
    for half in halves:
        h = half.core
        names.update({
            f"recv{h}": pltpu.VMEM((n_tp * half.d_tok, some, wide), BF16),
            f"slot_in{h}": pltpu.VMEM((n_tp, half.d_slot, some, wide), BF16),
            f"acc{h}": pltpu.VMEM((2, some, units), F32),
            f"hid{h}": pltpu.VMEM((some, units), BF16),
            f"ysend{h}": pltpu.VMEM((n_tp * items, some, wide), BF16),
            f"in_slot{h}": pltpu.VMEM((half.r_slot, n_tp + 1, some, wide), BF16),
            f"zs_send{h}": dma((2, n_tp, half.d_slot)),
            f"zs_recv{h}": dma((n_tp, half.d_slot)),
            f"xr{h}": dma((n_tp * half.d_tok + half.d_slot,)),
            f"ys{h}": dma((n_tp * half.r_tok + half.r_slot,)),
            f"ps_send{h}": dma((n_tp, half.r_slot)),
            f"ps_recv{h}": dma((2, n_tp, half.r_slot)),
        })
    return names


def body(names, halves, n_ep, n_tp, rows, width, cap, wide, *refs):
    tok_hbm, gain_ref, ids_ref, prob_ref, gate_hbm, up_hbm, down_hbm, out_hbm = refs[:8]
    r = dict(zip(names, refs[8:]))
    tok, send, ret, in_tok, part = (r[n] for n in ("tok", "send", "ret", "in_tok", "part"))
    w_gate, w_up, w_down = r["w_gate"], r["w_up"], r["w_down"]
    dmat, wmat, stats, rowscale = r["dmat"], r["wmat"], r["stats"], r["rowscale"]
    e, z = lax.axis_index("ep"), lax.axis_index("tp")
    core, seat = lax.rem(e, 2), e // 2
    last = n_tp - 1
    items = width // wide
    slots, n_src = n_ep * cap, n_ep // 2
    table = near_first(n_tp)

    def nth(k):
        return look_up(table, z * n_tp + k)

    def far(k):
        return nth(last - k)

    def column(s, m):
        return pl.multiple_of(s * width + m * wide, wide)

    def block(i):
        return pl.ds(pl.multiple_of(i * cap, cap), cap)

    def mine(half):
        return core == half.core

    def remote(axis, index, src, dst, send_sem, recv_sem):
        return pltpu.make_async_remote_copy(
            src_ref=src,
            dst_ref=dst,
            send_sem=send_sem,
            recv_sem=recv_sem,
            device_id={axis: index},
            device_id_type=pl.DeviceIdType.MESH,
        )

    def awaited(ref, count, send_sem, recv_sem):
        some = ref.at[pl.ds(0, count)]
        return remote("ep", lax.rem(e + 1, n_ep), some, some, send_sem, recv_sem)

    def repeat(first, past, fn):
        if past <= UNROLL:
            for i in range(first, past):
                fn(i)
        else:
            pl.loop(first, past)(fn)

    def each_peer(fn):
        repeat(1, n_ep, lambda shift: fn(lax.rem(e + shift, n_ep)))

    def next_to(way):
        return lax.rem(z + n_tp - 1 if way == 0 else z + 1, n_tp)

    loads = [
        pltpu.make_async_copy(
            tok_hbm.at[:, pl.ds(m * wide, wide)], tok.at[z, m], r["load_sem"].at[m]
        )
        for m in range(items)
    ]
    weights = [
        pltpu.make_async_copy(src, dst, r["load_sem"].at[items + i])
        for i, (src, dst) in enumerate(
            ((gate_hbm, w_gate), (up_hbm, w_up), (down_hbm, w_down))
        )
    ]
    for copy in loads + weights:
        copy.start()

    barrier = pltpu.get_barrier_semaphore()

    def greet(axis, index):
        pl.semaphore_signal(
            barrier, inc=1, device_id={axis: index}, device_id_type=pl.DeviceIdType.MESH
        )

    each_peer(lambda p: greet("ep", p))
    for shift in range(1, n_tp):
        greet("tp", lax.rem(z + shift, n_tp))

    ids = ids_ref[...].T
    prob = prob_ref[...].astype(F32).T
    lane = lax.broadcasted_iota(jnp.int32, (rows, 128), 1)
    picked = jnp.zeros((rows, 128), F32)
    chance = jnp.zeros((rows, 128), F32)
    for k in range(TOP):
        same = ids[:, k : k + 1] == lane
        picked = jnp.where(same, 1.0, picked)
        chance = jnp.where(same, prob[:, k : k + 1], chance)
    picked = picked.astype(BF16)
    earlier = (
        lax.broadcasted_iota(jnp.int32, (rows, rows), 1)
        < lax.broadcasted_iota(jnp.int32, (rows, rows), 0)
    )
    earlier = jnp.where(earlier, 1.0, 0.0).astype(BF16)
    before = jnp.dot(earlier, picked, preferred_element_type=F32).astype(BF16)
    spread_row = lax.broadcasted_iota(jnp.int32, (128, slots), 0)
    spread_col = lax.broadcasted_iota(jnp.int32, (128, slots), 1)
    spread = jnp.where(
        (spread_col >= spread_row * cap) & (spread_col < (spread_row + 1) * cap), 1.0, 0.0
    ).astype(BF16)
    is_picked = jnp.dot(picked, spread, preferred_element_type=F32)
    place = jnp.dot(before, spread, preferred_element_type=F32)
    weight = jnp.dot(chance.astype(BF16), spread, preferred_element_type=F32)
    position = lax.rem(lax.broadcasted_iota(jnp.int32, (rows, slots), 1), cap).astype(F32)
    hit = (is_picked > 0.5) & (place == position)
    wmat[...] = jnp.where(hit, weight, 0.0).astype(BF16)
    dmat[...] = jnp.where(hit, 1.0, 0.0).T.astype(BF16)

    pl.semaphore_wait(barrier, n_ep - 1 + n_tp - 1)

    def along(way, s, m):
        return remote(
            "tp", next_to(way), tok.at[s, m], tok.at[s, m],
            r["zt_send"].at[way, s, m], r["zt_recv"].at[s, m],
        )

    def along_slot(half, way, s, a):
        h = half.core
        ref = r[f"slot_in{h}"].at[s, a]
        return remote(
            "tp", next_to(way), ref, ref,
            r[f"zs_send{h}"].at[way, s, a], r[f"zs_recv{h}"].at[s, a],
        )

    def both_ways(copy):
        @pl.when(z > 0)
        def _():
            copy(0).start()

        @pl.when(z < last)
        def _():
            copy(1).start()

    square = jnp.zeros((rows, wide), F32)
    gain = gain_ref[...].astype(F32).reshape(1, width)
    for m in range(items):
        loads[m].wait()
        values = tok[z, m].astype(F32)
        square = square + values * values
        tok[z, m] = (values * gain[:, m * wide : (m + 1) * wide]).astype(BF16)
        if m < halves[0].d_tok:
            @pl.when(mine(halves[0]))
            def _():
                both_ways(lambda way: along(way, z, m))

    square = jnp.sum(square, axis=1, keepdims=True)
    stats[z] = jnp.broadcast_to(square, (rows, 128)).T[0:8, :]

    def share(shift):
        ref = stats.at[z]
        peer = lax.rem(z + shift, n_tp)
        return remote("tp", peer, ref, ref, r["st_send"].at[shift], r["st_recv"].at[shift])

    for shift in range(1, n_tp):
        share(shift).start()

    def dispatch(half, s, m, index, dst):
        placed = jnp.dot(dmat[...], tok[s, m], preferred_element_type=F32)
        send[index] = placed.astype(BF16)
        dst[block(seat), :] = send[index, block(e), :]
        sems = r["xs"].at[index], r[f"xr{half.core}"].at[index]
        each_peer(
            lambda p: remote("ep", p, send.at[index, block(p)], dst.at[block(seat)], *sems).start()
        )

    def wait_in(half, index, dst):
        sems = r["xs"].at[index], r[f"xr{half.core}"].at[index]

        @pl.when(mine(half))
        def _():
            awaited(dst, (n_src - 1) * cap, *sems).wait_recv()

        @pl.when(core != half.core)
        def _():
            awaited(dst, n_src * cap, *sems).wait_recv()

    def wait_out(half):
        @pl.when(mine(half))
        def _():
            @pl.loop(0, n_tp * half.d_tok + half.d_slot)
            def _(i):
                sem = r["xs"].at[i]
                awaited(send.at[i], (n_ep - 1) * cap, sem, sem).wait_send()

    def gate_up(half, chunk, row, first=False):
        acc = r[f"acc{half.core}"]
        values = chunk[...]
        at = pl.ds(row, wide)
        for i, matrix in enumerate((w_gate, w_up)):
            product = jnp.dot(values, matrix[at, :], preferred_element_type=F32)
            acc[i] = product if first else acc[i] + product

    def slot_ref(half):
        slot_in = r[f"slot_in{half.core}"]
        return lambda s, a: slot_in.at[s, a]

    def own_slots_out(half):
        @pl.when(mine(half))
        def _():
            for a in range(half.d_slot):
                index = n_tp * half.d_tok + a
                dispatch(half, z, half.d_tok + a, index, slot_ref(half)(z, a))

    def own_toks_out(half):
        @pl.when(mine(half))
        def _():
            @pl.loop(0, half.d_tok)
            def _(j):
                dispatch(half, z, j, j, r[f"recv{half.core}"].at[j])

    def own_slots_in(half):
        for a in range(half.d_slot):
            ref = slot_ref(half)(z, a)
            wait_in(half, n_tp * half.d_tok + a, ref)
            both_ways(lambda way: along_slot(half, way, z, a))

    def own_slots_used(half):
        for a in range(half.d_slot):
            gate_up(half, slot_ref(half)(z, a), column(z, half.d_tok + a), first=a == 0)

    def arrive(k, copy):
        @pl.when(z + k <= last)
        def _():
            copy(0, z + k).wait_recv()

            @pl.when(z > 0)
            def _():
                copy(0, z + k).start()

        @pl.when(z - k >= 0)
        def _():
            copy(1, z - k).wait_recv()

            @pl.when(z < last)
            def _():
                copy(1, z - k).start()

    def tok_on(half, k, j):
        @pl.when(mine(half))
        def _():
            arrive(k, lambda way, s: along(way, s, j))
            index = k * half.d_tok + j
            dispatch(half, nth(k), j, index, r[f"recv{half.core}"].at[index])

    def slots_on(half, k):
        for a in range(half.d_slot):
            arrive(k, lambda way, s: along_slot(half, way, s, a))

    def slots_used(half, k):
        s = nth(k)
        for a in range(half.d_slot):
            gate_up(half, slot_ref(half)(s, a), column(s, half.d_tok + a))

    def take_in(half, k, j):
        index = k * half.d_tok + j
        ref = r[f"recv{half.core}"].at[index]
        wait_in(half, index, ref)
        gate_up(half, ref, column(nth(k), j))

    def take_in_all(half, first, past):
        @pl.loop(first * half.d_tok, past * half.d_tok)
        def _(i):
            take_in(half, i // half.d_tok, lax.rem(i, half.d_tok))

    def hidden(half):
        h = half.core
        scale = r["slotscale"][h, :, 0:1]
        gate_act = r[f"acc{h}"][0] * scale
        up_act = r[f"acc{h}"][1] * scale
        r[f"hid{h}"][...] = (gate_act / (1.0 + jnp.exp(-gate_act)) * up_act).astype(BF16)

    def scale_to(p):
        ref = rowscale.at[e]
        return remote("ep", p, ref, ref, r["sc_send"].at[0], r["sc_recv"].at[0])

    def all_scales():
        return awaited(rowscale, n_ep - 1, r["sc_send"].at[0], r["sc_recv"].at[0])

    def send_scales():
        for shift in range(1, n_tp):
            share(shift).wait_recv()
        total = stats[0]
        for i in range(1, n_tp):
            total = total + stats[i]
        factor = lax.rsqrt(total / (width * n_tp) + EPSILON)
        by_slot = lax.dot_general(
            factor,
            dmat[...].astype(F32),
            (((1,), (1,)), ((), ())),
            precision=lax.Precision.HIGHEST,
            preferred_element_type=F32,
        )
        rowscale[e] = by_slot[0:1, :]
        each_peer(lambda p: scale_to(p).start())

    def turn_scales():
        all_scales().wait_recv()
        for source in range(n_ep):
            r["turned"][...] = jnp.broadcast_to(rowscale[source], (8, slots)).T
            own = r["turned"][block(e), 0:1]
            at = source // 2 * cap
            r["slotscale"][source % 2, at : at + cap, :] = jnp.broadcast_to(own, (cap, 128))

    def down(half, index, s, m):
        matrix = w_down[:, pl.ds(column(s, m), wide)]
        h = half.core
        r[f"ysend{h}"][index] = jnp.dot(
            r[f"hid{h}"][...], matrix, preferred_element_type=F32
        ).astype(BF16)

    def to_owners(half, index, slot):
        ysend = r[f"ysend{half.core}"]
        sems = r[f"ys{half.core}"].at[slot], r["yr"].at[slot]

        def to_seat(shift):
            q = lax.rem(seat + shift, n_src)
            remote(
                "ep", 2 * q + half.core, ysend.at[index, block(q)], ret.at[slot, block(e)], *sems
            ).start()

        @pl.when(mine(half))
        def _():
            ret[slot, block(e), :] = ysend[index, block(seat), :]

        @pl.when(core != half.core)
        def _():
            to_seat(0)

        repeat(1, n_src, to_seat)

    def sent_to_owners(half, slot):
        sem = r[f"ys{half.core}"].at[slot]
        ref = r[f"ysend{half.core}"].at[0]

        @pl.when(mine(half))
        def _():
            awaited(ref, (n_src - 1) * cap, sem, sem).wait_send()

        @pl.when(core != half.core)
        def _():
            awaited(ref, n_src * cap, sem, sem).wait_send()

    def seat_of(way, s):
        if way == 0:
            return s
        return s + (n_tp - s) * (1 - (z - 1 - s + n_tp - 1) // n_tp)

    def onward(way, k, s, m, src):
        return remote(
            "tp", next_to(1 - way), src, in_tok.at[m, seat_of(way, s)],
            r["pt_send"].at[k, m], r["pt_recv"].at[way, s, m],
        )

    def onward_slot(half, way, k, s, a, src):
        h = half.core
        return remote(
            "tp", next_to(1 - way), src, r[f"in_slot{h}"].at[a, seat_of(way, s)],
            r[f"ps_send{h}"].at[k, a], r[f"ps_recv{h}"].at[way, s, a],
        )

    def slot_index(half, k, a):
        return n_tp * half.r_tok + k * half.r_slot + a

    def toks_down(half, first, past):
        @pl.loop(first * half.r_tok, past * half.r_tok)
        def _(i):
            down(half, i, far(i // half.r_tok), lax.rem(i, half.r_tok))
            to_owners(half, i, i)

    def slots_down(half, first, past):
        @pl.loop(first, past)
        def _(k):
            for a in range(half.r_slot):
                s, index = far(k), slot_index(half, k, a)
                down(half, index, s, half.r_tok + a)
                ref = r[f"ysend{half.core}"].at[index]

                @pl.when((z == 0) & (k < last))
                def _():
                    onward_slot(half, 0, k, s, a, ref).start()

                @pl.when((z == last) & (k < last))
                def _():
                    onward_slot(half, 1, k, s, a, ref).start()

    def slots_pass(half, k):
        ysend, in_slot = r[f"ysend{half.core}"], r[f"in_slot{half.core}"]
        s = far(k)
        for a in range(half.r_slot):
            index = slot_index(half, k, a)

            def pass_on(way):
                copy = onward_slot(half, way, k, s, a, ysend.at[index])
                awaited_here = remote(
                    "tp", next_to(way), in_slot.at[a, s], in_slot.at[a, s],
                    r[f"ps_send{half.core}"].at[k, a], r[f"ps_recv{half.core}"].at[way, s, a],
                )
                awaited_here.wait_recv()
                summed = ysend[index].astype(F32) + in_slot[a, s].astype(F32)
                ysend[index] = summed.astype(BF16)
                copy.start()

            @pl.when((s > z) & (z > 0))
            def _():
                pass_on(0)

            @pl.when((s < z) & (z < last))
            def _():
                pass_on(1)

    def own_slots_back(half):
        ysend, in_slot = r[f"ysend{half.core}"], r[f"in_slot{half.core}"]
        for a in range(half.r_slot):
            index = slot_index(half, last, a)

            def add(way, at):
                ref = in_slot.at[a, at]
                remote(
                    "tp", next_to(way), ref, ref,
                    r[f"ps_send{half.core}"].at[0, a], r[f"ps_recv{half.core}"].at[way, z, a],
                ).wait_recv()
                summed = ysend[index].astype(F32) + in_slot[a, at].astype(F32)
                ysend[index] = summed.astype(BF16)

            @pl.when(z > 0)
            def _():
                add(0, z)

            @pl.when(z < last)
            def _():
                add(1, n_tp)

            to_owners(half, index, n_tp * half.r_tok + a)

    def combine(i):
        sem = r["yr"].at[i]
        awaited(ret.at[i], (n_ep - 1) * cap, sem, sem).wait_recv()
        return jnp.dot(wmat[...], ret[i], preferred_element_type=F32)

    def add_in(way, s, at, j):
        ref = in_tok.at[j, at]
        remote(
            "tp", next_to(way), ref, ref, r["pt_send"].at[0, j], r["pt_recv"].at[way, s, j]
        ).wait_recv()
        part[...] = part[...] + in_tok[j, at].astype(F32)

    def parts_on(half, first, past, where=True):
        @pl.when(mine(half) & where)
        def _():
            @pl.loop(first * half.r_tok, past * half.r_tok)
            def _(i):
                k, j = i // half.r_tok, lax.rem(i, half.r_tok)
                s = far(k)
                part[...] = combine(i)

                @pl.when((s > z) & (z > 0))
                def _():
                    add_in(0, s, s, j)

                @pl.when((s < z) & (z < last))
                def _():
                    add_in(1, s, s, j)

                send[i, 0:rows, :] = part[...].astype(BF16)
                ref = send.at[i, pl.ds(0, rows)]

                @pl.when(s > z)
                def _():
                    onward(0, k, s, j, ref).start()

                @pl.when(s < z)
                def _():
                    onward(1, k, s, j, ref).start()

    def write(m):
        columns = pl.ds(pl.multiple_of(m * wide, wide), wide)
        return pltpu.make_async_copy(r["result"].at[m], out_hbm.at[:, columns], r["out_sem"].at[m])

    def finish(half):
        @pl.when(mine(half))
        def _():
            @pl.loop(0, half.r_tok)
            def _(j):
                part[...] = combine(last * half.r_tok + j)

                @pl.when(z > 0)
                def _():
                    add_in(0, z, z, j)

                @pl.when(z < last)
                def _():
                    add_in(1, z, n_tp, j)

                r["result"][j] = part[...].astype(BF16)

                @pl.when(j > 0)
                def _():
                    write(j - 1).start()

            for a in range(half.r_slot):
                m = half.r_tok + a
                r["result"][m] = combine(n_tp * half.r_tok + a).astype(BF16)
                write(m - 1).start()

            write(items - 1).start()

    def toks_on(half, k):
        @pl.loop(0, half.d_tok)
        def _(j):
            tok_on(half, k, j)

    one, two = halves
    at_end = (z == 0) | (z == last)
    inside = (z > 0) & (z < last)

    own_slots_out(one)
    own_toks_out(one)
    weights[0].wait()
    weights[1].wait()
    own_slots_in(one)
    own_slots_used(one)

    @pl.loop(one.d_tok, n_tp * one.d_tok)
    def _(i):
        k, j = i // one.d_tok, lax.rem(i, one.d_tok)
        tok_on(one, k, j)
        take_in(one, k - 1, j)

        @pl.when((j == one.d_tok - 1) & (k < last))
        def _():
            slots_on(one, k)

        @pl.when(i == 2 * one.d_tok - 1)
        def _():
            send_scales()

    @pl.when(mine(two))
    def _():
        for m in range(two.d_tok):
            both_ways(lambda way: along(way, z, m))

    own_slots_out(two)
    turn_scales()

    @pl.loop(1, last)
    def _(k):
        slots_used(one, k)

    take_in_all(one, last, n_tp)
    own_toks_out(two)
    slots_on(one, last)
    slots_used(one, last)
    own_slots_in(two)
    hidden(one)
    weights[2].wait()
    wait_out(one)

    slots_down(one, 0, 1)
    toks_down(one, 0, 1)
    toks_on(two, 1)
    slots_down(one, 1, n_tp)
    toks_down(one, 1, last)
    own_slots_used(two)
    take_in_all(two, 0, 1)
    if last > 1:
        slots_on(two, 1)
        slots_used(two, 1)
    for k in range(2, n_tp):
        slots_pass(one, k - 2)
        toks_on(two, k)
        if k < last:
            parts_on(one, k - 2, k - 1, at_end)
    slots_pass(one, last - 1)
    parts_on(one, max(0, last - 2), last, at_end)
    for k in range(2, last):
        slots_on(two, k)
        slots_used(two, k)
    take_in_all(two, 1, last - 1)
    own_slots_back(one)
    toks_down(one, last, n_tp)
    parts_on(one, 0, 1, inside)
    take_in_all(two, last - 1, last)
    parts_on(one, 1, last - 1, inside)
    take_in_all(two, last, n_tp)
    slots_on(two, last)
    slots_used(two, last)
    hidden(two)
    wait_out(two)

    toks_down(two, 0, 1)
    slots_down(two, 0, n_tp)
    parts_on(one, last - 1, last, inside)
    toks_down(two, 1, n_tp)
    finish(one)
    for k in range(last):
        slots_pass(two, k)
    parts_on(two, 0, 1)
    own_slots_back(two)

    all_scales().wait_send()
    for shift in range(1, n_tp):
        share(shift).wait_send()

    def onward_done(half):
        @pl.loop(0, last)
        def _(k):
            for a in range(half.r_slot):
                onward_slot(half, 0, k, 0, a, r[f"ysend{half.core}"].at[0]).wait_send()

    def parts_done(half, first, past):
        @pl.when(mine(half))
        def _():
            @pl.loop(first, past)
            def _(k):
                for m in range(half.r_tok):
                    onward(0, k, 0, m, send.at[0, pl.ds(0, rows)]).wait_send()

    def owners_done(half, first, past):
        @pl.loop(first, past)
        def _(i):
            sent_to_owners(half, i)

    for half in halves:
        @pl.loop(0, n_tp)
        def _(s):
            for way, sends in enumerate(((z > 0) & (s >= z), (z < last) & (s <= z))):
                @pl.when(sends)
                def _():
                    for a in range(half.d_slot):
                        along_slot(half, way, s, a).wait_send()

                    @pl.when(mine(half))
                    def _():
                        for m in range(half.d_tok):
                            along(way, s, m).wait_send()

    owners_done(one, 0, n_tp * one.r_tok + one.r_slot)
    onward_done(one)
    parts_done(one, 0, last)
    parts_on(two, 1, last)
    owners_done(two, 0, last * two.r_tok)
    onward_done(two)
    parts_done(two, 0, last - 1)
    finish(two)
    parts_done(two, last - 1, last)
    owners_done(two, last * two.r_tok, n_tp * two.r_tok + two.r_slot)
    for m in range(items):
        write(m).wait()


def local(tokens, norm_gain, expert_ids, gate_prob, w_gate, w_up, w_down):
    n_ep = lax.axis_size("ep")
    n_tp = lax.axis_size("tp")
    rows, width = tokens.shape
    cap = max(2, 2 * rows * TOP // (EXP_DEV * n_ep))
    wide = 256 if width % 256 == 0 else 128
    halves = [Half(core, width // wide) for core in range(2)]
    names = buffers(n_ep, n_tp, rows, width, cap, wide, w_gate.shape[2], halves)
    kernel = functools.partial(
        body, list(names), halves, n_ep, n_tp, rows, width, cap, wide
    )
    vmem = pl.BlockSpec(memory_space=pltpu.VMEM)
    hbm = pl.BlockSpec(memory_space=pl.ANY)
    return pl.pallas_call(
        kernel,
        out_shape=jax.ShapeDtypeStruct((rows, width), BF16),
        in_specs=[hbm, vmem, vmem, vmem, hbm, hbm, hbm],
        out_specs=hbm,
        scratch_shapes=list(names.values()),
        compiler_params=pltpu.CompilerParams(
            collective_id=0, has_side_effects=True, vmem_limit_bytes=67043328
        ),
        name="moe",
    )(
        tokens,
        norm_gain,
        expert_ids.T,
        gate_prob.T,
        w_gate[0],
        w_up[0],
        w_down[0],
    )


def solution(mesh):
    placed = (
        P("ep", "tp"),
        P("tp"),
        P("ep", None),
        P("ep", None),
        P("ep", None, "tp"),
        P("ep", None, "tp"),
        P("ep", "tp", None),
    )
    return jax.shard_map(
        local, mesh=mesh, in_specs=placed, out_specs=P("ep", "tp"), check_vma=False
    )
```

```python
import functools

import jax
import jax.numpy as jnp
from jax import lax
from jax.experimental import pallas as pl
from jax.experimental.pallas import tpu as pltpu
from jax.sharding import PartitionSpec as P

TOP = 8
EXP_DEV = 8
SHARES = ((1, 3), (3, 1))
PARTS = 7
UNROLL = 8
EPSILON = 1e-06
BF16 = jnp.bfloat16
F32 = jnp.float32


def look_up(table, index):
    span = len(table) ** 2
    total = 0
    for i, value in enumerate(table):
        if value:
            total = total + value * (1 - ((index - i) * (index - i) + span - 1) // span)
    return total


def near_first(n_tp):
    table = []
    for z in range(n_tp):
        inner = 1 if z < n_tp / 2 else -1
        table += sorted(range(n_tp), key=lambda s: (abs(s - z), -inner * (s - z)))
    return table


class Half:
    def __init__(self, core, items):
        forth, back = (max(1, items * share // PARTS) for share in SHARES[core])
        self.core = core
        self.d_slot, self.d_tok = forth, items - forth
        self.r_slot, self.r_tok = back, items - back


def buffers(n_ep, n_tp, rows, width, cap, wide, units, halves):
    items = width // wide
    slots, some = n_ep * cap, n_ep // 2 * cap
    most_d = max(n_tp * half.d_tok + half.d_slot for half in halves)
    most_r = max(n_tp * half.r_tok + half.r_slot for half in halves)
    most_tok = max(half.r_tok for half in halves)
    dma = pltpu.SemaphoreType.DMA
    names = dict(
        tok=pltpu.VMEM((n_tp, items, rows, wide), BF16),
        stats=pltpu.VMEM((n_tp, 8, rows), F32),
        rowscale=pltpu.VMEM((n_ep, 1, slots), F32),
        turned=pltpu.VMEM((slots, 8), F32),
        slotscale=pltpu.VMEM((2, some, 128), F32),
        dmat=pltpu.VMEM((slots, rows), BF16),
        wmat=pltpu.VMEM((rows, slots), BF16),
        send=pltpu.VMEM((most_d, slots, wide), BF16),
        w_gate=pltpu.VMEM((n_tp * width, units), BF16),
        w_up=pltpu.VMEM((n_tp * width, units), BF16),
        w_down=pltpu.VMEM((units, n_tp * width), BF16),
        ret=pltpu.VMEM((most_r, slots, wide), BF16),
        in_tok=pltpu.VMEM((most_tok, n_tp + 1, rows, wide), BF16),
        part=pltpu.VMEM((rows, wide), F32),
        result=pltpu.VMEM((items, rows, wide), BF16),
        load_sem=dma((items + 3,)),
        out_sem=dma((items,)),
        st_send=dma((1,)),
        st_recv=dma((1,)),
        sc_send=dma((1,)),
        sc_recv=dma((1,)),
        zt_send=dma((2, n_tp)),
        zt_recv=dma((n_tp, items)),
        xs=dma((1,)),
        yr=dma((most_r,)),
        pt_send=dma((1,)),
        pt_recv=dma((n_tp + 1, most_tok)),
    )
    for half in halves:
        h = half.core
        names.update({
            f"recv{h}": pltpu.VMEM((n_tp * half.d_tok, some, wide), BF16),
            f"slot_in{h}": pltpu.VMEM((n_tp, half.d_slot, some, wide), BF16),
            f"acc{h}": pltpu.VMEM((2, some, units), F32),
            f"hid{h}": pltpu.VMEM((some, units), BF16),
            f"ysend{h}": pltpu.VMEM((n_tp * items, some, wide), BF16),
            f"in_slot{h}": pltpu.VMEM((half.r_slot, n_tp + 1, some, wide), BF16),
            f"zs_send{h}": dma((2, n_tp)),
            f"zs_recv{h}": dma((n_tp, half.d_slot)),
            f"xr{h}": dma((n_tp * half.d_tok + half.d_slot,)),
            f"ys{h}": dma((1,)),
            f"ps_send{h}": dma((1,)),
            f"ps_recv{h}": dma((n_tp + 1, half.r_slot)),
        })
    return names


def body(names, halves, n_ep, n_tp, rows, width, cap, wide, *refs):
    tok_hbm, gain_ref, ids_ref, prob_ref, gate_hbm, up_hbm, down_hbm, out_hbm = refs[:8]
    r = dict(zip(names, refs[8:]))
    tok, send, ret, in_tok, part = (r[n] for n in ("tok", "send", "ret", "in_tok", "part"))
    w_gate, w_up, w_down = r["w_gate"], r["w_up"], r["w_down"]
    dmat, wmat, stats, rowscale = r["dmat"], r["wmat"], r["stats"], r["rowscale"]
    e, z = lax.axis_index("ep"), lax.axis_index("tp")
    core, seat = lax.rem(e, 2), e // 2
    last = n_tp - 1
    items = width // wide
    slots, n_src = n_ep * cap, n_ep // 2
    table = near_first(n_tp)

    def nth(k):
        return look_up(table, z * n_tp + k)

    def far(k):
        return nth(last - k)

    def column(s, m):
        return pl.multiple_of(s * width + m * wide, wide)

    def block(i):
        return pl.ds(pl.multiple_of(i * cap, cap), cap)

    def mine(half):
        return core == half.core

    def remote(axis, index, src, dst, send_sem, recv_sem):
        return pltpu.make_async_remote_copy(
            src_ref=src,
            dst_ref=dst,
            send_sem=send_sem,
            recv_sem=recv_sem,
            device_id={axis: index},
            device_id_type=pl.DeviceIdType.MESH,
        )

    def awaited(ref, count, send_sem, recv_sem):
        some = ref.at[pl.ds(0, count)]
        return remote("ep", lax.rem(e + 1, n_ep), some, some, send_sem, recv_sem)

    def repeat(first, past, fn):
        if past <= UNROLL:
            for i in range(first, past):
                fn(i)
        else:
            pl.loop(first, past)(fn)

    def sent(buffer, chunks, count, sem):
        some = buffer.at[pl.ds(0, chunks), pl.ds(0, count)]
        remote("ep", lax.rem(e + 1, n_ep), some, some, sem, sem).wait_send()

    def each_peer(fn):
        repeat(1, n_ep, lambda shift: fn(lax.rem(e + shift, n_ep)))

    def next_to(way):
        return lax.rem(z + n_tp - 1 if way == 0 else z + 1, n_tp)

    loads = [
        pltpu.make_async_copy(
            tok_hbm.at[:, pl.ds(m * wide, wide)], tok.at[z, m], r["load_sem"].at[m]
        )
        for m in range(items)
    ]
    weights = [
        pltpu.make_async_copy(src, dst, r["load_sem"].at[items + i])
        for i, (src, dst) in enumerate(
            ((gate_hbm, w_gate), (up_hbm, w_up), (down_hbm, w_down))
        )
    ]
    for copy in loads + weights:
        copy.start()

    barrier = pltpu.get_barrier_semaphore()

    def greet(axis, index):
        pl.semaphore_signal(
            barrier, inc=1, device_id={axis: index}, device_id_type=pl.DeviceIdType.MESH
        )

    each_peer(lambda p: greet("ep", p))
    for shift in range(1, n_tp):
        greet("tp", lax.rem(z + shift, n_tp))

    ids = ids_ref[...].T
    prob = prob_ref[...].astype(F32).T
    lane = lax.broadcasted_iota(jnp.int32, (rows, 128), 1)
    picked = jnp.zeros((rows, 128), F32)
    chance = jnp.zeros((rows, 128), F32)
    for k in range(TOP):
        same = ids[:, k : k + 1] == lane
        picked = jnp.where(same, 1.0, picked)
        chance = jnp.where(same, prob[:, k : k + 1], chance)
    picked = picked.astype(BF16)
    earlier = (
        lax.broadcasted_iota(jnp.int32, (rows, rows), 1)
        < lax.broadcasted_iota(jnp.int32, (rows, rows), 0)
    )
    earlier = jnp.where(earlier, 1.0, 0.0).astype(BF16)
    before = jnp.dot(earlier, picked, preferred_element_type=F32).astype(BF16)
    spread_row = lax.broadcasted_iota(jnp.int32, (128, slots), 0)
    spread_col = lax.broadcasted_iota(jnp.int32, (128, slots), 1)
    spread = jnp.where(
        (spread_col >= spread_row * cap) & (spread_col < (spread_row + 1) * cap), 1.0, 0.0
    ).astype(BF16)
    is_picked = jnp.dot(picked, spread, preferred_element_type=F32)
    place = jnp.dot(before, spread, preferred_element_type=F32)
    weight = jnp.dot(chance.astype(BF16), spread, preferred_element_type=F32)
    position = lax.rem(lax.broadcasted_iota(jnp.int32, (rows, slots), 1), cap).astype(F32)
    hit = (is_picked > 0.5) & (place == position)
    wmat[...] = jnp.where(hit, weight, 0.0).astype(BF16)
    dmat[...] = jnp.where(hit, 1.0, 0.0).T.astype(BF16)

    pl.semaphore_wait(barrier, n_ep - 1 + n_tp - 1)

    def along(way, s, m):
        return remote(
            "tp", next_to(way), tok.at[s, m], tok.at[s, m],
            r["zt_send"].at[way, s], r["zt_recv"].at[s, m],
        )

    def along_slot(half, way, s, a):
        h = half.core
        ref = r[f"slot_in{h}"].at[s, a]
        return remote(
            "tp", next_to(way), ref, ref,
            r[f"zs_send{h}"].at[way, s], r[f"zs_recv{h}"].at[s, a],
        )

    def both_ways(copy):
        @pl.when(z > 0)
        def _():
            copy(0).start()

        @pl.when(z < last)
        def _():
            copy(1).start()

    square = jnp.zeros((rows, wide), F32)
    gain = gain_ref[...].astype(F32).reshape(1, width)
    for m in range(items):
        loads[m].wait()
        values = tok[z, m].astype(F32)
        square = square + values * values
        tok[z, m] = (values * gain[:, m * wide : (m + 1) * wide]).astype(BF16)
        if m < halves[0].d_tok:
            @pl.when(mine(halves[0]))
            def _():
                both_ways(lambda way: along(way, z, m))

    square = jnp.sum(square, axis=1, keepdims=True)
    stats[z] = jnp.broadcast_to(square, (rows, 128)).T[0:8, :]

    def share(shift):
        ref = stats.at[z]
        peer = lax.rem(z + shift, n_tp)
        return remote("tp", peer, ref, ref, r["st_send"].at[0], r["st_recv"].at[0])

    for shift in range(1, n_tp):
        share(shift).start()

    def shares():
        return awaited(stats, last, r["st_send"].at[0], r["st_recv"].at[0])

    def dispatch(half, s, m, index, dst):
        placed = jnp.dot(dmat[...], tok[s, m], preferred_element_type=F32)
        send[index] = placed.astype(BF16)
        dst[block(seat), :] = send[index, block(e), :]
        sems = r["xs"].at[0], r[f"xr{half.core}"].at[index]
        each_peer(
            lambda p: remote("ep", p, send.at[index, block(p)], dst.at[block(seat)], *sems).start()
        )

    def wait_in(half, index, dst):
        sems = r["xs"].at[0], r[f"xr{half.core}"].at[index]

        @pl.when(mine(half))
        def _():
            awaited(dst, (n_src - 1) * cap, *sems).wait_recv()

        @pl.when(core != half.core)
        def _():
            awaited(dst, n_src * cap, *sems).wait_recv()

    def wait_out(half):
        @pl.when(mine(half))
        def _():
            sent(send, n_tp * half.d_tok + half.d_slot, (n_ep - 1) * cap, r["xs"].at[0])

    def gate_up(half, chunk, row, first=False):
        acc = r[f"acc{half.core}"]
        values = chunk[...]
        at = pl.ds(row, wide)
        for i, matrix in enumerate((w_gate, w_up)):
            product = jnp.dot(values, matrix[at, :], preferred_element_type=F32)
            acc[i] = product if first else acc[i] + product

    def slot_ref(half):
        slot_in = r[f"slot_in{half.core}"]
        return lambda s, a: slot_in.at[s, a]

    def own_slots_out(half):
        @pl.when(mine(half))
        def _():
            for a in range(half.d_slot):
                index = n_tp * half.d_tok + a
                dispatch(half, z, half.d_tok + a, index, slot_ref(half)(z, a))

    def own_toks_out(half):
        @pl.when(mine(half))
        def _():
            @pl.loop(0, half.d_tok)
            def _(j):
                dispatch(half, z, j, j, r[f"recv{half.core}"].at[j])

    def own_slots_in(half):
        for a in range(half.d_slot):
            ref = slot_ref(half)(z, a)
            wait_in(half, n_tp * half.d_tok + a, ref)
            both_ways(lambda way: along_slot(half, way, z, a))

    def own_slots_used(half):
        for a in range(half.d_slot):
            gate_up(half, slot_ref(half)(z, a), column(z, half.d_tok + a), first=a == 0)

    def arrive(k, copy):
        @pl.when(z + k <= last)
        def _():
            copy(0, z + k).wait_recv()

            @pl.when(z > 0)
            def _():
                copy(0, z + k).start()

        @pl.when(z - k >= 0)
        def _():
            copy(1, z - k).wait_recv()

            @pl.when(z < last)
            def _():
                copy(1, z - k).start()

    def tok_on(half, k, j):
        @pl.when(mine(half))
        def _():
            arrive(k, lambda way, s: along(way, s, j))
            index = k * half.d_tok + j
            dispatch(half, nth(k), j, index, r[f"recv{half.core}"].at[index])

    def slots_on(half, k):
        for a in range(half.d_slot):
            arrive(k, lambda way, s: along_slot(half, way, s, a))

    def slots_used(half, k):
        s = nth(k)
        for a in range(half.d_slot):
            gate_up(half, slot_ref(half)(s, a), column(s, half.d_tok + a))

    def take_in(half, k, j):
        index = k * half.d_tok + j
        ref = r[f"recv{half.core}"].at[index]
        wait_in(half, index, ref)
        gate_up(half, ref, column(nth(k), j))

    def take_in_all(half, first, past):
        @pl.loop(first * half.d_tok, past * half.d_tok)
        def _(i):
            take_in(half, i // half.d_tok, lax.rem(i, half.d_tok))

    def hidden(half):
        h = half.core
        scale = r["slotscale"][h, :, 0:1]
        gate_act = r[f"acc{h}"][0] * scale
        up_act = r[f"acc{h}"][1] * scale
        r[f"hid{h}"][...] = (gate_act / (1.0 + jnp.exp(-gate_act)) * up_act).astype(BF16)

    def scale_to(p):
        ref = rowscale.at[e]
        return remote("ep", p, ref, ref, r["sc_send"].at[0], r["sc_recv"].at[0])

    def all_scales():
        return awaited(rowscale, n_ep - 1, r["sc_send"].at[0], r["sc_recv"].at[0])

    def send_scales():
        shares().wait_recv()
        total = stats[0]
        for i in range(1, n_tp):
            total = total + stats[i]
        factor = lax.rsqrt(total / (width * n_tp) + EPSILON)
        by_slot = lax.dot_general(
            factor,
            dmat[...].astype(F32),
            (((1,), (1,)), ((), ())),
            precision=lax.Precision.HIGHEST,
            preferred_element_type=F32,
        )
        rowscale[e] = by_slot[0:1, :]
        each_peer(lambda p: scale_to(p).start())

    def turn_scales():
        all_scales().wait_recv()
        for source in range(n_ep):
            r["turned"][...] = jnp.broadcast_to(rowscale[source], (8, slots)).T
            own = r["turned"][block(e), 0:1]
            at = source // 2 * cap
            r["slotscale"][source % 2, at : at + cap, :] = jnp.broadcast_to(own, (cap, 128))

    def down(half, index, s, m):
        matrix = w_down[:, pl.ds(column(s, m), wide)]
        h = half.core
        r[f"ysend{h}"][index] = jnp.dot(
            r[f"hid{h}"][...], matrix, preferred_element_type=F32
        ).astype(BF16)

    def to_owners(half, index, slot):
        ysend = r[f"ysend{half.core}"]
        sems = r[f"ys{half.core}"].at[0], r["yr"].at[slot]

        def to_seat(shift):
            q = lax.rem(seat + shift, n_src)
            remote(
                "ep", 2 * q + half.core, ysend.at[index, block(q)], ret.at[slot, block(e)], *sems
            ).start()

        @pl.when(mine(half))
        def _():
            ret[slot, block(e), :] = ysend[index, block(seat), :]

        @pl.when(core != half.core)
        def _():
            to_seat(0)

        repeat(1, n_src, to_seat)

    def owners_done(half):
        sem = r[f"ys{half.core}"].at[0]
        ysend, chunks = r[f"ysend{half.core}"], n_tp * half.r_tok + half.r_slot

        @pl.when(mine(half))
        def _():
            sent(ysend, chunks, (n_src - 1) * cap, sem)

        @pl.when(core != half.core)
        def _():
            sent(ysend, chunks, n_src * cap, sem)

    def seat_of(way, s):
        if way == 0:
            return s
        return s + (n_tp - s) * (1 - (z - 1 - s + n_tp - 1) // n_tp)

    def onward(way, s, m, src):
        return remote(
            "tp", next_to(1 - way), src, in_tok.at[m, seat_of(way, s)],
            r["pt_send"].at[0], r["pt_recv"].at[seat_of(way, s), m],
        )

    def onward_slot(half, way, s, a, src):
        h = half.core
        return remote(
            "tp", next_to(1 - way), src, r[f"in_slot{h}"].at[a, seat_of(way, s)],
            r[f"ps_send{h}"].at[0], r[f"ps_recv{h}"].at[seat_of(way, s), a],
        )

    def slot_index(half, k, a):
        return n_tp * half.r_tok + k * half.r_slot + a

    def toks_down(half, first, past):
        @pl.loop(first * half.r_tok, past * half.r_tok)
        def _(i):
            down(half, i, far(i // half.r_tok), lax.rem(i, half.r_tok))
            to_owners(half, i, i)

    def slots_down(half, first, past):
        @pl.loop(first, past)
        def _(k):
            for a in range(half.r_slot):
                s, index = far(k), slot_index(half, k, a)
                down(half, index, s, half.r_tok + a)
                ref = r[f"ysend{half.core}"].at[index]

                @pl.when((z == 0) & (k < last))
                def _():
                    onward_slot(half, 0, s, a, ref).start()

                @pl.when((z == last) & (k < last))
                def _():
                    onward_slot(half, 1, s, a, ref).start()

    def slots_pass(half, k):
        ysend, in_slot = r[f"ysend{half.core}"], r[f"in_slot{half.core}"]
        s = far(k)
        for a in range(half.r_slot):
            index = slot_index(half, k, a)

            def pass_on(way):
                copy = onward_slot(half, way, s, a, ysend.at[index])
                awaited_here = remote(
                    "tp", next_to(way), in_slot.at[a, s], in_slot.at[a, s],
                    r[f"ps_send{half.core}"].at[0], r[f"ps_recv{half.core}"].at[s, a],
                )
                awaited_here.wait_recv()
                summed = ysend[index].astype(F32) + in_slot[a, s].astype(F32)
                ysend[index] = summed.astype(BF16)
                copy.start()

            @pl.when((s > z) & (z > 0))
            def _():
                pass_on(0)

            @pl.when((s < z) & (z < last))
            def _():
                pass_on(1)

    def own_slots_back(half):
        ysend, in_slot = r[f"ysend{half.core}"], r[f"in_slot{half.core}"]
        for a in range(half.r_slot):
            index = slot_index(half, last, a)

            def add(way, at):
                ref = in_slot.at[a, at]
                remote(
                    "tp", next_to(way), ref, ref,
                    r[f"ps_send{half.core}"].at[0], r[f"ps_recv{half.core}"].at[at, a],
                ).wait_recv()
                summed = ysend[index].astype(F32) + in_slot[a, at].astype(F32)
                ysend[index] = summed.astype(BF16)

            @pl.when(z > 0)
            def _():
                add(0, z)

            @pl.when(z < last)
            def _():
                add(1, n_tp)

            to_owners(half, index, n_tp * half.r_tok + a)

    def combine(i):
        sem = r["yr"].at[i]
        awaited(ret.at[i], (n_ep - 1) * cap, sem, sem).wait_recv()
        return jnp.dot(wmat[...], ret[i], preferred_element_type=F32)

    def add_in(way, at, j):
        ref = in_tok.at[j, at]
        remote(
            "tp", next_to(way), ref, ref, r["pt_send"].at[0], r["pt_recv"].at[at, j]
        ).wait_recv()
        part[...] = part[...] + in_tok[j, at].astype(F32)

    def parts_on(half, first, past, where=True):
        @pl.when(mine(half) & where)
        def _():
            @pl.loop(first * half.r_tok, past * half.r_tok)
            def _(i):
                k, j = i // half.r_tok, lax.rem(i, half.r_tok)
                s = far(k)
                part[...] = combine(i)

                @pl.when((s > z) & (z > 0))
                def _():
                    add_in(0, s, j)

                @pl.when((s < z) & (z < last))
                def _():
                    add_in(1, s, j)

                send[i, 0:rows, :] = part[...].astype(BF16)
                ref = send.at[i, pl.ds(0, rows)]

                @pl.when(s > z)
                def _():
                    onward(0, s, j, ref).start()

                @pl.when(s < z)
                def _():
                    onward(1, s, j, ref).start()

    def write(m):
        columns = pl.ds(pl.multiple_of(m * wide, wide), wide)
        return pltpu.make_async_copy(r["result"].at[m], out_hbm.at[:, columns], r["out_sem"].at[m])

    def finish(half):
        @pl.when(mine(half))
        def _():
            @pl.loop(0, half.r_tok)
            def _(j):
                part[...] = combine(last * half.r_tok + j)

                @pl.when(z > 0)
                def _():
                    add_in(0, z, j)

                @pl.when(z < last)
                def _():
                    add_in(1, n_tp, j)

                r["result"][j] = part[...].astype(BF16)

                @pl.when(j > 0)
                def _():
                    write(j - 1).start()

            for a in range(half.r_slot):
                m = half.r_tok + a
                r["result"][m] = combine(n_tp * half.r_tok + a).astype(BF16)
                write(m - 1).start()

            write(items - 1).start()

    def toks_on(half, k):
        @pl.loop(0, half.d_tok)
        def _(j):
            tok_on(half, k, j)

    one, two = halves
    at_end = (z == 0) | (z == last)
    inside = (z > 0) & (z < last)

    own_slots_out(one)
    own_toks_out(one)
    weights[0].wait()
    weights[1].wait()
    own_slots_in(one)
    own_slots_used(one)

    @pl.loop(one.d_tok, n_tp * one.d_tok)
    def _(i):
        k, j = i // one.d_tok, lax.rem(i, one.d_tok)
        tok_on(one, k, j)
        take_in(one, k - 1, j)

        @pl.when((j == one.d_tok - 1) & (k < last))
        def _():
            slots_on(one, k)

        @pl.when(i == 2 * one.d_tok - 1)
        def _():
            send_scales()

    @pl.when(mine(two))
    def _():
        for m in range(two.d_tok):
            both_ways(lambda way: along(way, z, m))

    own_slots_out(two)
    turn_scales()

    @pl.loop(1, last)
    def _(k):
        slots_used(one, k)

    take_in_all(one, last, n_tp)
    own_toks_out(two)
    slots_on(one, last)
    slots_used(one, last)
    own_slots_in(two)
    hidden(one)
    weights[2].wait()
    wait_out(one)

    slots_down(one, 0, 1)
    toks_down(one, 0, 1)
    toks_on(two, 1)
    slots_down(one, 1, n_tp)
    toks_down(one, 1, last)
    own_slots_used(two)
    take_in_all(two, 0, 1)
    if last > 1:
        slots_on(two, 1)
        slots_used(two, 1)
    for k in range(2, n_tp):
        slots_pass(one, k - 2)
        toks_on(two, k)
        if k < last:
            parts_on(one, k - 2, k - 1, at_end)
    slots_pass(one, last - 1)
    parts_on(one, max(0, last - 2), last, at_end)
    for k in range(2, last):
        slots_on(two, k)
        slots_used(two, k)
    take_in_all(two, 1, last - 1)
    own_slots_back(one)
    toks_down(one, last, n_tp)
    parts_on(one, 0, 1, inside)
    take_in_all(two, last - 1, last)
    parts_on(one, 1, last - 1, inside)
    take_in_all(two, last, n_tp)
    slots_on(two, last)
    slots_used(two, last)
    hidden(two)
    wait_out(two)

    toks_down(two, 0, 1)
    slots_down(two, 0, n_tp)
    parts_on(one, last - 1, last, inside)
    toks_down(two, 1, n_tp)
    finish(one)
    for k in range(last):
        slots_pass(two, k)
    parts_on(two, 0, 1)
    own_slots_back(two)

    all_scales().wait_send()
    shares().wait_send()

    def onward_done(half):
        chunks = last * half.r_slot
        sent(r[f"ysend{half.core}"], chunks, n_src * cap, r[f"ps_send{half.core}"].at[0])

    def parts_done(half):
        @pl.when(mine(half))
        def _():
            sent(send, last * half.r_tok, rows, r["pt_send"].at[0])

    for half in halves:
        @pl.loop(0, n_tp)
        def _(s):
            for way, sends in enumerate(((z > 0) & (s >= z), (z < last) & (s <= z))):
                @pl.when(sends)
                def _():
                    h = half.core
                    awaited(
                        r[f"slot_in{h}"].at[s], half.d_slot,
                        r[f"zs_send{h}"].at[way, s], r[f"zs_recv{h}"].at[s, 0],
                    ).wait_send()

                    @pl.when(mine(half))
                    def _():
                        awaited(
                            tok.at[s], half.d_tok, r["zt_send"].at[way, s], r["zt_recv"].at[s, 0]
                        ).wait_send()

    owners_done(one)
    onward_done(one)
    parts_done(one)
    parts_on(two, 1, last)
    onward_done(two)
    finish(two)
    parts_done(two)
    owners_done(two)
    for m in range(items):
        write(m).wait()


def local(tokens, norm_gain, expert_ids, gate_prob, w_gate, w_up, w_down):
    n_ep = lax.axis_size("ep")
    n_tp = lax.axis_size("tp")
    rows, width = tokens.shape
    cap = max(2, 2 * rows * TOP // (EXP_DEV * n_ep))
    wide = 256 if width % 256 == 0 else 128
    halves = [Half(core, width // wide) for core in range(2)]
    names = buffers(n_ep, n_tp, rows, width, cap, wide, w_gate.shape[2], halves)
    kernel = functools.partial(
        body, list(names), halves, n_ep, n_tp, rows, width, cap, wide
    )
    vmem = pl.BlockSpec(memory_space=pltpu.VMEM)
    hbm = pl.BlockSpec(memory_space=pl.ANY)
    return pl.pallas_call(
        kernel,
        out_shape=jax.ShapeDtypeStruct((rows, width), BF16),
        in_specs=[hbm, vmem, vmem, vmem, hbm, hbm, hbm],
        out_specs=hbm,
        scratch_shapes=list(names.values()),
        compiler_params=pltpu.CompilerParams(
            collective_id=0, has_side_effects=True, vmem_limit_bytes=67043328
        ),
        name="moe",
    )(
        tokens,
        norm_gain,
        expert_ids.T,
        gate_prob.T,
        w_gate[0],
        w_up[0],
        w_down[0],
    )


def solution(mesh):
    placed = (
        P("ep", "tp"),
        P("tp"),
        P("ep", None),
        P("ep", None),
        P("ep", None, "tp"),
        P("ep", None, "tp"),
        P("ep", "tp", None),
    )
    return jax.shard_map(
        local, mesh=mesh, in_specs=placed, out_specs=P("ep", "tp"), check_vma=False
    )
```
